512 devices in a mesh: uly: 8 (over y, core), blk: 64 (over x, z).
Axes of the slice: x: 4, y: 4, z: 16, core: 2. Of those that a mesh axis runs over, the one named last changes fastest.
Arguments:
- query_inputs: bfloat16 [65536, 2048], P(('blk', 'uly')), may hold values from -6 to 6
- key_inputs: bfloat16 [65536, 1024], P(('blk', 'uly')), may hold values from -6 to 6
- value_inputs: bfloat16 [65536, 1024], P(('blk', 'uly')), may hold values from -6 to 6
- forward_out: bfloat16 [65536, 2048], P(('blk', 'uly')), may hold values from -6 to 6
- output_gradient: bfloat16 [65536, 2048], P(('blk', 'uly')), may hold values from -4 to 4
- lse_parts: float32 [65536, 16, 2], P(('blk', 'uly')), may hold values from 3 to 247
- segment_ids: int32 [65536], P(('blk', 'uly')), may hold values from 0 to 127, never falling along the last dimension, each value on 1 to 2048 neighbouring positions
Outputs:
- query_grad: bfloat16 [65536, 2048], P(('blk', 'uly'))
- key_grad: bfloat16 [65536, 1024], P(('blk', 'uly'))
- value_grad: bfloat16 [65536, 1024], P(('blk', 'uly'))
The draws below stay inside these ranges and needn't reach their ends.
Inputs may be any that keep to these rules, and one draw needn't show every extreme that they name: `segment_ids`: never falls along the sequence; every document holds 1 to 2048 tokens, and some document exactly 2048.
All inputs are finite; a program needn't handle non-finite values.
Results may differ from the reference program's by a relative error of at most 0.0051.
Values may be sent and summed in bfloat16 or wider, within the bound.
A program may use at most 128 MiB of HBM per device.

```python
import math
import jax
import jax.numpy as jnp
import numpy as np
from jax import lax

HEAD_SIZE = 128
QUERY_HEADS = 16
KEY_VALUE_HEADS = 8
QBLOCK = 512
SEQUENCE_TOKENS = 65536
DOCUMENT_LIMIT = 2048
SEGS = 128


def draw_lse_parts(key, part):
    first_key = jax.random.fold_in(key, 0)
    shape_all = (SEQUENCE_TOKENS, QUERY_HEADS, 2)
    return jnp.clip(5.0 + 0.8 * jax.random.normal(first_key, shape_all, jnp.float32), 3.0, 7.0)


def shard_levels(key, dims, cuts, least, top_value):
    def one(dim, shards_of):
        draws = jax.random.uniform(jax.random.fold_in(jax.random.fold_in(key, 6), dim), (shards_of,), jnp.float32, least / len(cuts), top_value / len(cuts))
        return jnp.repeat(jnp.exp(draws), dims[dim] // shards_of).reshape((-1,) + (1,) * (len(dims) - dim - 1))

    loudness = one(*cuts[0])
    for cut in cuts[1:]:
        loudness = loudness * one(*cut)
    return loudness


def split_up(count, total, most, slope):
    loads = [(1 << 20) // math.isqrt(grade ** slope) + 1 for grade in range(2, count + 1)]
    rest, counts = total - most - (count - 1), [1] * (count - 1)
    while rest > 0:
        candidates = [i for i in range(count - 1) if counts[i] < most]
        pool, budget = sum([loads[i] for i in candidates]), rest
        for i in candidates:
            extra = min(most - counts[i], max(1, budget * loads[i] // pool), rest)
            counts[i] = counts[i] + extra
            rest = rest - extra
    return np.array([most] + counts)


def ragged_sizes(rng, number_of, total, bound, slope):
    if number_of == 2:
        one = jax.random.randint(rng, (), max(1, total - bound), min(bound, total - 1) + 1)
        return jnp.stack([one, total - one])
    sizes = jnp.asarray(split_up(number_of, total, bound, slope), jnp.int32)
    pairs = (number_of - 1) // 2
    donor, taker = sizes[1:1 + 2 * pairs:2], sizes[2:2 + 2 * pairs:2]
    room = jnp.minimum(donor - 1, bound - taker)
    passed = jax.random.randint(jax.random.fold_in(rng, 1), (pairs,), 0, 1 << 20) % (room + 1)
    sizes = sizes.at[1:1 + 2 * pairs:2].set(donor - passed).at[2:2 + 2 * pairs:2].set(taker + passed)
    return sizes[jax.random.permutation(jax.random.fold_in(rng, 2), number_of)]


def scatter_about(rng, extent, deviation, limit, cuts=(), kind=jnp.bfloat16):
    array = jax.random.normal(rng, extent, jnp.float32) * deviation
    if len(cuts) > 0:
        array = shard_levels(rng, extent, cuts, -0.22, 0.18) * array
    return jnp.clip(array, min=-limit, max=limit).astype(kind)


def setup_inputs(seed: int = 0) -> dict:
    keys = jax.random.split(jax.random.key(seed), 8)
    return {
        "query_inputs": scatter_about(keys[0], (SEQUENCE_TOKENS, QUERY_HEADS * HEAD_SIZE), 1.0, 6.0, ((0, 512),)),
        "key_inputs": scatter_about(keys[1], (SEQUENCE_TOKENS, KEY_VALUE_HEADS * HEAD_SIZE), 1.0, 6.0, ((0, 512),)),
        "value_inputs": scatter_about(keys[2], (SEQUENCE_TOKENS, KEY_VALUE_HEADS * HEAD_SIZE), 1.0, 6.0, ((0, 512),)),
        "forward_out": scatter_about(keys[3], (SEQUENCE_TOKENS, QUERY_HEADS * HEAD_SIZE), 0.5, 6.0, ((0, 512),)),
        "output_gradient": scatter_about(keys[4], (SEQUENCE_TOKENS, QUERY_HEADS * HEAD_SIZE), 0.25, 4.0, ((0, 512),)),
        "lse_parts": draw_lse_parts(jax.random.fold_in(keys[7], 71), 0),
        "segment_ids": jnp.searchsorted(jnp.cumsum(ragged_sizes(keys[6], SEGS, SEQUENCE_TOKENS, DOCUMENT_LIMIT, 2)), jnp.arange(SEQUENCE_TOKENS), side="right").astype(jnp.int32),
    }


def merge_parts(partials):
    highest = lax.optimization_barrier(jnp.max(partials, axis=-1))
    return highest + jnp.log(lax.optimization_barrier(jnp.sum(jnp.exp(partials - highest[..., None]), axis=-1)))

def round_trip(values_in):
    rounded = lax.optimization_barrier(values_in.astype(jnp.bfloat16))
    return rounded.astype(jnp.float32)

def reference(query_inputs, key_inputs, value_inputs, forward_out, output_gradient, lse_parts, segment_ids):
    token_count = query_inputs.shape[0]
    group_width = QUERY_HEADS // KEY_VALUE_HEADS
    score_scale = 1.0 / math.sqrt(HEAD_SIZE)
    rows_per_block = min(QBLOCK, token_count)
    lookback_span = DOCUMENT_LIMIT + rows_per_block
    logsumexp_rows = merge_parts(lse_parts)
    products = output_gradient.astype(jnp.float32) * forward_out.astype(jnp.float32)
    row_deltas = lax.optimization_barrier(jnp.sum(products.reshape(token_count, QUERY_HEADS, HEAD_SIZE), axis=-1))
    key_with_padding = jnp.pad(key_inputs, ((DOCUMENT_LIMIT, 0), (0, 0)))
    value_with_padding = jnp.pad(value_inputs, ((DOCUMENT_LIMIT, 0), (0, 0)))
    ids_padded = jnp.concatenate([jnp.full((DOCUMENT_LIMIT,), -1, jnp.int32), segment_ids.astype(jnp.int32)])

    def block_step(carried, block_index):
        key_gradient_running, value_gradient_running = carried
        leading_row = (block_index * rows_per_block).astype(jnp.int32)
        query_quad = lax.dynamic_slice_in_dim(query_inputs, leading_row, rows_per_block, 0).astype(jnp.float32).reshape(rows_per_block, KEY_VALUE_HEADS, group_width, HEAD_SIZE)
        gradient_quad = lax.dynamic_slice_in_dim(output_gradient, leading_row, rows_per_block, 0).astype(jnp.float32).reshape(rows_per_block, KEY_VALUE_HEADS, group_width, HEAD_SIZE)
        logsumexp_cube = lax.dynamic_slice_in_dim(logsumexp_rows, leading_row, rows_per_block, 0).reshape(rows_per_block, KEY_VALUE_HEADS, group_width).transpose(1, 2, 0)[..., None]
        delta_cube = lax.dynamic_slice_in_dim(row_deltas, leading_row, rows_per_block, 0).reshape(rows_per_block, KEY_VALUE_HEADS, group_width).transpose(1, 2, 0)[..., None]
        key_cube = lax.dynamic_slice_in_dim(key_with_padding, leading_row, lookback_span, 0).astype(jnp.float32).reshape(lookback_span, KEY_VALUE_HEADS, HEAD_SIZE)
        value_cube = lax.dynamic_slice_in_dim(value_with_padding, leading_row, lookback_span, 0).astype(jnp.float32).reshape(lookback_span, KEY_VALUE_HEADS, HEAD_SIZE)
        query_ids = lax.dynamic_slice_in_dim(segment_ids.astype(jnp.int32), leading_row, rows_per_block, 0)
        key_ids = lax.dynamic_slice_in_dim(ids_padded, leading_row, lookback_span, 0)
        query_pos = leading_row + DOCUMENT_LIMIT + jnp.arange(rows_per_block, dtype=jnp.int32)
        key_pos = leading_row + jnp.arange(lookback_span, dtype=jnp.int32)
        allowed = (key_pos[None, :] <= query_pos[:, None]) & (key_ids[None, :] == query_ids[:, None])
        scores = jnp.einsum('mhgd,nhd->hgmn', query_quad, key_cube) * score_scale
        weights = jnp.where(allowed, jnp.exp(scores - logsumexp_cube), 0.0)
        value_portion = jnp.einsum('hgmn,mhgd->nhd', round_trip(weights), gradient_quad)
        prob_grad = jnp.einsum('mhgd,nhd->hgmn', gradient_quad, value_cube)
        score_grad = round_trip(weights * (prob_grad - delta_cube))
        query_part = jnp.einsum('hgmn,nhd->mhgd', score_grad, key_cube) * score_scale
        key_portion = jnp.einsum('hgmn,mhgd->nhd', score_grad, query_quad) * score_scale
        key_window_rows = lax.dynamic_slice_in_dim(key_gradient_running, leading_row, lookback_span, 0) + key_portion.reshape(lookback_span, KEY_VALUE_HEADS * HEAD_SIZE)
        value_window_rows = lax.dynamic_slice_in_dim(value_gradient_running, leading_row, lookback_span, 0) + value_portion.reshape(lookback_span, KEY_VALUE_HEADS * HEAD_SIZE)
        key_gradient_running = lax.dynamic_update_slice_in_dim(key_gradient_running, key_window_rows, leading_row, 0)
        value_gradient_running = lax.dynamic_update_slice_in_dim(value_gradient_running, value_window_rows, leading_row, 0)
        return ((key_gradient_running, value_gradient_running), query_part.reshape(rows_per_block, QUERY_HEADS * HEAD_SIZE).astype(jnp.bfloat16))
    initial_running = (jnp.zeros((token_count + DOCUMENT_LIMIT, KEY_VALUE_HEADS * HEAD_SIZE), jnp.float32), jnp.zeros((token_count + DOCUMENT_LIMIT, KEY_VALUE_HEADS * HEAD_SIZE), jnp.float32))
    final_acc, query_blocks = lax.scan(block_step, initial_running, jnp.arange(token_count // rows_per_block, dtype=jnp.int32))
    query_grad = query_blocks.reshape(token_count, QUERY_HEADS * HEAD_SIZE)
    key_grad = final_acc[0][DOCUMENT_LIMIT:].astype(jnp.bfloat16)
    value_grad = final_acc[1][DOCUMENT_LIMIT:].astype(jnp.bfloat16)
    return (query_grad, key_grad, value_grad)
```

```python
import functools
import math

import jax
import jax.numpy as jnp
from jax import lax
from jax.experimental import pallas as pl
from jax.experimental.pallas import tpu as pltpu
from jax.sharding import PartitionSpec as P

HEAD_SIZE = 128
QUERY_HEADS = 16
KEY_VALUE_HEADS = 8
GROUP = QUERY_HEADS // KEY_VALUE_HEADS
PIECES = 2
FAR = 8192.0


def dot(a, b):
    return lax.dot_general(a, b, (((1,), (0,)), ((), ())), preferred_element_type=jnp.float32)


def kernel(
    uly_count, blk_count,
    q_hbm, do_hbm, k_hbm, v_hbm, out_hbm, lp_hbm, ids_hbm,
    dq_ref, dk_ref, dv_ref,
    q_in, do_in, k_in, v_in, out_in, lp_in, ids_in,
    qb, dob, kvb, stat_ref, statb,
    aug, kaug, vaug, qT, dT, kT, vT,
    dqa, dka, dva,
    retk, retq, ink, inq, dqs, dkvs,
    loc_sem, keep_sem,
    qd_s, qd_r, kv_s, kv_r, st_s, st_r,
    zq_s, zq_r, zk_s, zk_r, zst_s, zst_r,
    rk_s, rk_r, rq_s, rq_r, oq_s, oq_r, okv_s, okv_r,
):
    U, B = uly_count, blk_count
    T = q_hbm.shape[0]
    R = T * U
    D = HEAD_SIZE
    GD = GROUP * D
    H = R // 2
    bf, f32 = jnp.bfloat16, jnp.float32
    scale = 1.0 / math.sqrt(D)
    u = lax.axis_index("uly")
    b = lax.axis_index("blk")
    has_dn = b >= 1
    has_up = b + 1 < B
    mid = jnp.logical_and(has_dn, has_up)

    def at(blk, uly):
        return {"blk": blk, "uly": uly}

    def rcopy(src, dst, ssem, rsem, dev):
        return pltpu.make_async_remote_copy(
            src_ref=src, dst_ref=dst, send_sem=ssem, recv_sem=rsem,
            device_id=dev, device_id_type=pl.DeviceIdType.MESH,
        )

    def cols(first, width):
        return pl.ds(pl.multiple_of(first, 128), width)

    def rows(place, base=0):
        return pl.ds(pl.multiple_of(base + place * T, T), T)

    def each(low, high, step):
        def body(i, c):
            step(i)
            return c
        lax.fori_loop(low, high, body, 0)

    barrier = pltpu.get_barrier_semaphore()
    for k in range(1, U):
        pl.semaphore_signal(
            barrier, inc=1, device_id=at(b, lax.rem(u + k, U)), device_id_type=pl.DeviceIdType.MESH
        )

    @pl.when(has_up)
    def _():
        pl.semaphore_signal(barrier, inc=1, device_id=at(b + 1, u), device_id_type=pl.DeviceIdType.MESH)

    @pl.when(has_dn)
    def _():
        pl.semaphore_signal(barrier, inc=1, device_id=at(b - 1, u), device_id_type=pl.DeviceIdType.MESH)

    loads = [
        pltpu.make_async_copy(src, dst, loc_sem.at[i])
        for i, (src, dst) in enumerate([
            (q_hbm, q_in), (do_hbm, do_in), (k_hbm, k_in), (v_hbm, v_in),
            (out_hbm, out_in), (lp_hbm, lp_in), (ids_hbm, ids_in),
        ])
    ]
    own = [
        pltpu.make_async_copy(q_hbm.at[:, cols(u * GD, GD)], qb.at[rows(u), :], loc_sem.at[7]),
        pltpu.make_async_copy(do_hbm.at[:, cols(u * GD, GD)], dob.at[rows(u), :], loc_sem.at[8]),
        pltpu.make_async_copy(k_hbm.at[:, cols(u * D, D)], kvb.at[0, rows(u), :], loc_sem.at[9]),
        pltpu.make_async_copy(v_hbm.at[:, cols(u * D, D)], kvb.at[1, rows(u), :], loc_sem.at[10]),
    ]
    for copy in loads + own:
        copy.start()

    def clear(i):
        spot = pl.ds(pl.multiple_of(i * T, T), T)
        dqa[0, spot, :] = jnp.zeros((T, D), f32)
        dqa[1, spot, :] = jnp.zeros((T, D), f32)
        dka[:, spot] = jnp.zeros((D, T), f32)
        dva[:, spot] = jnp.zeros((D, T), f32)
        kaug[:, spot] = jnp.zeros((D, T), bf)

    each(0, 2 * U, clear)
    r8 = lax.broadcasted_iota(jnp.int32, (8, T), 0)
    ones_v = jnp.where(jnp.logical_and(r8 >= 4, r8 < 7), 1.0, 0.0)
    for i in range(H // T):
        vaug[:, i * T:(i + 1) * T] = jnp.concatenate(
            [ones_v, jnp.zeros((D - 8, T), f32)], axis=0
        ).astype(bf)

    for copy in loads[:4]:
        copy.wait()
    pl.semaphore_wait(barrier, U - 1 + has_up.astype(jnp.int32) + has_dn.astype(jnp.int32))

    def frm_of(k):
        return lax.rem(u + U - k, U)

    def qd_in(which, h, k, place, peer, dev):
        ref, buf = ((q_in, qb), (do_in, dob))[which]
        return rcopy(
            ref.at[:, cols(peer * GD + h * D, D)], buf.at[rows(place), h * D:(h + 1) * D],
            qd_s.at[which, h, k], qd_r.at[which, h, k], dev,
        )

    def kv_in(which, k, place, peer, dev):
        ref = (k_in, v_in)[which]
        return rcopy(
            ref.at[:, cols(peer * D, D)], kvb.at[which, rows(place), :],
            kv_s.at[which, k], kv_r.at[which, k], dev,
        )

    def st_in(k, place, peer, dev):
        return rcopy(stat_ref.at[peer], statb.at[0, place], st_s.at[k], st_r.at[k], dev)

    def send_qd(h):
        def one(k):
            to = lax.rem(u + k, U)
            for which in range(2):
                qd_in(which, h, k, u, to, at(b, to)).start()
        each(1, U, one)

    def send_kv(k):
        to = lax.rem(u + k, U)
        for which in range(2):
            kv_in(which, k, u, to, at(b, to)).start()

    send_qd(0)
    each(1, U, send_kv)
    send_qd(1)

    for copy in loads[4:]:
        copy.wait()
    lane = lax.broadcasted_iota(jnp.int32, (T, 128), 1)
    table = jnp.zeros((T, 128), f32)
    for h in range(QUERY_HEADS):
        piece = slice(h * D, (h + 1) * D)
        total = jnp.sum(
            do_in[:, piece].astype(f32) * out_in[:, piece].astype(f32), axis=1, keepdims=True
        )
        table = jnp.where(lane == h, total, table)
    table = table.T
    part0, part1 = lp_in[:, 0, :], lp_in[:, 1, :]
    highest = jnp.maximum(part0, part1)
    lse_rows = highest + jnp.log(jnp.exp(part0 - highest) + jnp.exp(part1 - highest))
    id_rows = jnp.broadcast_to(ids_in[...].astype(f32), (8 - 2 * GROUP, T))
    for p in range(U):
        pick = slice(p * GROUP, (p + 1) * GROUP)
        stat_ref[p] = jnp.concatenate([lse_rows[pick], table[pick], id_rows], axis=0)
    statb[0, u] = stat_ref[u]

    def send_st(k):
        to = lax.rem(u + k, U)
        st_in(k, u, to, at(b, to)).start()

    each(1, U, send_st)

    def zq(which, h, place):
        buf = (qb, dob)[which]
        return rcopy(
            buf.at[rows(place), h * D:(h + 1) * D], buf.at[rows(place, R), h * D:(h + 1) * D],
            zq_s.at[which, h, place], zq_r.at[which, h, place], at(b - 1, u),
        )

    def zk(which, place):
        return rcopy(
            kvb.at[which, rows(place), :], kvb.at[which, rows(place, R), :],
            zk_s.at[which, place], zk_r.at[which, place], at(b + 1, u),
        )

    def zst(which):
        dev = (at(b - 1, u), at(b + 1, u))[which]
        return rcopy(statb.at[0], statb.at[1 + which], zst_s.at[which], zst_r.at[which], dev)

    lower = b >= 2

    def relay_q(h, place):
        @pl.when(lower)
        def _():
            for which in range(2):
                zq(which, h, place).start()

    def relay_k(place):
        @pl.when(has_up)
        def _():
            for which in range(2):
                zk(which, place).start()

    def turn_q(h, base):
        def one(p):
            spot = rows(p, base)
            qT[h, :, spot] = qb[spot, h * D:(h + 1) * D].T
            dT[h, :, spot] = dob[spot, h * D:(h + 1) * D].T
        each(0, U, one)

    def turn_k(base):
        def one(p):
            spot = rows(p, base)
            kT[:, spot] = kvb[0, spot, :].T
            vT[:, spot] = kvb[1, spot, :].T
        each(0, U, one)

    def codes(st):
        doc = jnp.broadcast_to(st[4:5, :], (16, T))
        high = jnp.floor(doc * 0.125)
        low = (doc - 8.0 * high)[:8]
        i16 = lax.broadcasted_iota(jnp.int32, (16, T), 0).astype(f32)
        return jnp.where(i16[:8] == low, 1.0, 0.0), jnp.where(i16 == high, 1.0, 0.0)

    def split3(x):
        a = x.astype(bf).astype(f32)
        c = (x - a).astype(bf).astype(f32)
        return a, c, (x - a - c)

    def build_q(which):
        def one(p):
            st = statb[which, p]
            oc, oa = codes(st)
            for h in range(GROUP):
                rows8 = jnp.ones((8, T), f32)
                parts = split3(st[h:h + 1, :] * (-math.sqrt(D)))
                more = split3(-st[GROUP + h:GROUP + h + 1, :])
                for i in range(3):
                    rows8 = jnp.where(r8 == i, parts[i], rows8)
                    rows8 = jnp.where(r8 == 4 + i, more[i], rows8)
                full = jnp.concatenate([rows8, oc, oa, jnp.zeros((D - 32, T), f32)], axis=0)
                aug[h, rows(p, which * R), :] = full.T.astype(bf)
        each(0, U, one)

    def build_k(src, base):
        def one(p):
            oc, oa = codes(statb[src, p])
            rows8 = jnp.where(r8 < 3, 1.0, jnp.where(r8 == 3, -2.0 * FAR, 0.0))
            kaug[0:32, rows(p, base)] = jnp.concatenate(
                [rows8, oc * FAR, oa * FAR], axis=0
            ).astype(bf)
        each(0, U, one)

    own[0].wait()
    own[1].wait()
    relay_q(0, u)

    def got_q(h):
        def one(k):
            frm = frm_of(k)
            for which in range(2):
                qd_in(which, h, k, frm, frm, at(b, frm)).wait_recv()
            relay_q(h, frm)
        each(1, U, one)

    got_q(0)
    own[2].wait()
    own[3].wait()
    relay_k(u)
    relay_q(1, u)
    turn_q(0, 0)

    def got_k(k):
        frm = frm_of(k)
        for which in range(2):
            kv_in(which, k, frm, frm, at(b, frm)).wait_recv()
        relay_k(frm)

    each(1, U, got_k)
    turn_k(0)
    got_q(1)

    def got_st(k):
        frm = frm_of(k)
        st_in(k, frm, frm, at(b, frm)).wait_recv()

    each(1, U, got_st)

    @pl.when(lower)
    def _():
        zst(0).start()

    @pl.when(has_up)
    def _():
        zst(1).start()

    turn_q(1, 0)
    build_q(0)
    build_k(0, 0)

    factor = scale * math.log2(math.e)

    def tile(qi, ki, causal):
        qrow = pl.ds(pl.multiple_of(qi * H, H), H)
        krow = pl.ds(pl.multiple_of(ki * H, H), H)
        ks = jnp.concatenate([kT[:, krow], kaug[:, krow]], axis=0)
        vs = jnp.concatenate([vT[:, krow], vaug[...]], axis=0)
        kn = kvb[0, krow, :]
        dk = dv = None
        for h in range(GROUP):
            extra = aug[h, qrow, :]
            qs = jnp.concatenate([qb[qrow, h * D:(h + 1) * D], extra], axis=1)
            ds = jnp.concatenate([dob[qrow, h * D:(h + 1) * D], extra], axis=1)
            w = jnp.exp2(dot(qs, ks) * factor)
            if causal:
                qpos = lax.broadcasted_iota(jnp.int32, (H, H), 0) + qi * H
                kpos = lax.broadcasted_iota(jnp.int32, (H, H), 1) + ki * H
                w = jnp.where(kpos <= qpos, w, 0.0)
            g = (w * dot(ds, vs)).astype(bf)
            w = w.astype(bf)
            part_v = dot(dT[h, :, qrow], w)
            part_k = dot(qT[h, :, qrow], g)
            dqa[h, qrow, :] += dot(g, kn)
            dv = part_v if dv is None else dv + part_v
            dk = part_k if dk is None else dk + part_k
        dva[:, krow] += dv
        dka[:, krow] += dk

    def near(t):
        tile((t + 1) // 2, t // 2, True)

    each(0, 3, near)

    def give_k(half):
        return rcopy(retk.at[half], ink.at[half], rk_s.at[half], rk_r.at[half], at(b - 1, u))

    def give_q(half):
        return rcopy(retq.at[half], inq.at[half], rq_s.at[half], rq_r.at[half], at(b + 1, u))

    def half_of(half, base=0):
        return slice(base + half * H, base + (half + 1) * H)

    @pl.when(has_dn)
    def _():
        zst(1).wait_recv()

        def one(p):
            for which in range(2):
                zk(which, p).wait_recv()
        each(0, U, one)
        turn_k(R)
        build_k(2, R)
        each(0, 2, lambda t: tile(t, 3, False))

    @pl.when(mid)
    def _():
        zst(0).wait_recv()

        def one(p):
            for h in range(GROUP):
                for which in range(2):
                    zq(which, h, p).wait_recv()
        each(0, U, one)
        for h in range(GROUP):
            turn_q(h, R)
        build_q(1)
        each(0, 2, lambda t: tile(3 - t, 3, False))
        retq[1] = dqa[:, half_of(1, R), :].astype(bf)
        give_q(1).start()

    @pl.when(has_dn)
    def _():
        retk[1, 0] = dka[:, half_of(1, R)].astype(bf)
        retk[1, 1] = dva[:, half_of(1, R)].astype(bf)
        give_k(1).start()
        each(0, jnp.where(has_up, 3, 2), lambda t: tile(t, 2, False))
        retk[0, 0] = dka[:, half_of(0, R)].astype(bf)
        retk[0, 1] = dva[:, half_of(0, R)].astype(bf)
        give_k(0).start()

    @pl.when(mid)
    def _():
        retq[0] = dqa[:, half_of(0, R), :].astype(bf)
        give_q(0).start()

    def oq(place, peer, dev):
        return rcopy(
            dqs.at[rows(place), :], dq_ref.at[:, cols(peer * GD, GD)],
            oq_s.at[place], oq_r.at[peer], dev,
        )

    def okv(which, place, peer, dev):
        ref = (dk_ref, dv_ref)[which]
        return rcopy(
            dkvs.at[which, rows(place), :], ref.at[:, cols(peer * D, D)],
            okv_s.at[which, place], okv_r.at[which, peer], dev,
        )

    def keep_q():
        return pltpu.make_async_copy(
            dqs.at[rows(u), :], dq_ref.at[:, cols(u * GD, GD)], keep_sem.at[2]
        )

    def keep_kv(which):
        ref = (dk_ref, dv_ref)[which]
        return pltpu.make_async_copy(
            dkvs.at[which, rows(u), :], ref.at[:, cols(u * D, D)], keep_sem.at[which]
        )

    Q = U // 2

    def spread(half, start_remote, start_own):
        mine = (u // Q) == half
        for k in range(Q):
            to = half * Q + lax.rem(lax.rem(u, Q) + k, Q)
            if k == 0:
                @pl.when(mine)
                def _():
                    start_own()

                @pl.when(jnp.logical_not(mine))
                def _():
                    start_remote(to)
            else:
                start_remote(to)

    def finish_q(half):
        @pl.when(lower)
        def _():
            give_q(half).wait_recv()
            for h in range(GROUP):
                dqa[h, half_of(half), :] += inq[half, h].astype(f32)
        for h in range(GROUP):
            dqs[half_of(half), h * D:(h + 1) * D] = (dqa[h, half_of(half), :] * scale).astype(bf)
        spread(half, lambda to: oq(to, u, at(b, to)).start(), lambda: keep_q().start())

    def finish_kv(half):
        @pl.when(has_up)
        def _():
            give_k(half).wait_recv()
            dka[:, half_of(half)] += ink[half, 0].astype(f32)
            dva[:, half_of(half)] += ink[half, 1].astype(f32)
        dkvs[0, half_of(half), :] = (dka[:, half_of(half)] * scale).T.astype(bf)
        dkvs[1, half_of(half), :] = dva[:, half_of(half)].T.astype(bf)

        def go(to):
            for which in range(2):
                okv(which, to, u, at(b, to)).start()

        def stay():
            for which in range(2):
                keep_kv(which).start()

        spread(half, go, stay)

    for half in (1, 0):
        finish_q(half)
        finish_kv(half)

    keep_q().wait()
    for which in range(2):
        keep_kv(which).wait()

    def drain(k):
        to, frm = lax.rem(u + k, U), frm_of(k)
        for which in range(2):
            for h in range(GROUP):
                qd_in(which, h, k, u, to, at(b, to)).wait_send()
            kv_in(which, k, u, to, at(b, to)).wait_send()
        st_in(k, u, to, at(b, to)).wait_send()
        oq(to, u, at(b, to)).wait_send()
        oq(u, frm, at(b, frm)).wait_recv()
        for which in range(2):
            okv(which, to, u, at(b, to)).wait_send()
            okv(which, u, frm, at(b, frm)).wait_recv()

    each(1, U, drain)

    @pl.when(lower)
    def _():
        zst(0).wait_send()

        def one(p):
            for which in range(2):
                for h in range(GROUP):
                    zq(which, h, p).wait_send()
        each(0, U, one)

    @pl.when(has_up)
    def _():
        zst(1).wait_send()

        def one(p):
            for which in range(2):
                zk(which, p).wait_send()
        each(0, U, one)

    @pl.when(has_dn)
    def _():
        for half in range(2):
            give_k(half).wait_send()

    @pl.when(mid)
    def _():
        for half in range(2):
            give_q(half).wait_send()


def close_kernel(a_in, b_in, c_in, a_out, b_out, c_out, a_mid, b_mid, c_mid, in_sem, out_sem):
    moves = []
    for i, (src, mid, dst) in enumerate(
        [(a_in, a_mid, a_out), (b_in, b_mid, b_out), (c_in, c_mid, c_out)]
    ):
        height = src.shape[0] // PIECES
        for n in range(PIECES):
            part = pl.ds(n * height, height)
            moves.append((
                pltpu.make_async_copy(src.at[part], mid.at[part], in_sem.at[i, n]),
                pltpu.make_async_copy(mid.at[part], dst.at[part], out_sem.at[i, n]),
            ))
    for load, _ in moves:
        load.start()
    for load, store in moves:
        load.wait()
        store.start()
    for _, store in moves:
        store.wait()


def per_device(uly_count, blk_count, q, k, v, out, grad, lse_parts, segment_ids):
    U, B = uly_count, blk_count
    T = q.shape[0]
    R = T * U
    D = HEAD_SIZE
    GD = GROUP * D
    assert KEY_VALUE_HEADS == U
    parts = lse_parts.transpose(1, 2, 0)
    ids = segment_ids.reshape(1, T)
    bf, f32 = jnp.bfloat16, jnp.float32
    dma = pltpu.SemaphoreType.DMA
    sems = []
    for shape in [(2, 2, U), (2, U), (U,), (2, 2, U), (2, U), (2,), (2,), (2,), (U,), (2, U)]:
        sems += [dma(shape), dma(shape)]
    vm = pltpu.VMEM
    results = pl.pallas_call(
        functools.partial(kernel, U, B),
        out_shape=(
            jax.ShapeDtypeStruct(q.shape, bf),
            jax.ShapeDtypeStruct(k.shape, bf),
            jax.ShapeDtypeStruct(v.shape, bf),
        ),
        in_specs=[pl.BlockSpec(memory_space=pltpu.HBM)] * 7,
        out_specs=tuple([pl.BlockSpec(memory_space=pltpu.HBM)] * 3),
        scratch_shapes=[
            vm(q.shape, bf), vm(q.shape, bf), vm(k.shape, bf), vm(v.shape, bf),
            vm(q.shape, bf), vm(parts.shape, f32), vm((1, T), jnp.int32),
            vm((2 * R, GD), bf), vm((2 * R, GD), bf), vm((2, 2 * R, D), bf),
            vm((U, 8, T), f32), vm((3, U, 8, T), f32),
            vm((GROUP, 2 * R, D), bf), vm((D, 2 * R), bf), vm((D, R // 2), bf),
            vm((GROUP, D, 2 * R), bf), vm((GROUP, D, 2 * R), bf),
            vm((D, 2 * R), bf), vm((D, 2 * R), bf),
            vm((GROUP, 2 * R, D), f32), vm((D, 2 * R), f32), vm((D, 2 * R), f32),
            vm((2, 2, D, R // 2), bf), vm((2, GROUP, R // 2, D), bf),
            vm((2, 2, D, R // 2), bf), vm((2, GROUP, R // 2, D), bf),
            vm((R, GD), bf), vm((2, R, D), bf),
            dma((11,)), dma((3,)),
        ] + sems,
        compiler_params=pltpu.CompilerParams(
            collective_id=0, has_side_effects=True, vmem_limit_bytes=60 << 20
        ),
    )(q, grad, k, v, out, parts, ids)
    hbm = [pl.BlockSpec(memory_space=pltpu.HBM)] * 3
    return pl.pallas_call(
        close_kernel,
        out_shape=tuple(jax.ShapeDtypeStruct(r.shape, r.dtype) for r in results),
        in_specs=hbm,
        out_specs=tuple(hbm),
        scratch_shapes=[vm(r.shape, r.dtype) for r in results]
        + [dma((3, PIECES)), dma((3, PIECES))],
        compiler_params=pltpu.CompilerParams(vmem_limit_bytes=56 << 20),
    )(*results)


def solution(mesh):
    spec = P(("blk", "uly"), None)
    body = functools.partial(per_device, mesh.shape["uly"], mesh.shape["blk"])
    return jax.shard_map(
        body,
        mesh=mesh,
        in_specs=(spec, spec, spec, spec, spec, P(("blk", "uly"), None, None), P(("blk", "uly"))),
        out_specs=(spec, spec, spec),
        check_vma=False,
    )
```

```python
import functools
import math

import jax
import jax.numpy as jnp
from jax import lax
from jax.experimental import pallas as pl
from jax.experimental.pallas import tpu as pltpu
from jax.sharding import PartitionSpec as P

HEAD_SIZE = 128
QUERY_HEADS = 16
KEY_VALUE_HEADS = 8
GROUP = QUERY_HEADS // KEY_VALUE_HEADS
PIECES = 2
FAR = 8192.0
LAYER = 16


def dot(a, b):
    return lax.dot_general(a, b, (((1,), (0,)), ((), ())), preferred_element_type=jnp.float32)


def kernel(
    uly_count, blk_count,
    q_hbm, do_hbm, k_hbm, v_hbm, out_hbm, lp_hbm, ids_hbm,
    dq_ref, dk_ref, dv_ref,
    q_in, do_in, k_in, v_in, out_in, lp_in, ids_in,
    qb, dob, kvb, stat_ref, statb,
    aug, kaug, vaug, qT, dT, kT, vT,
    dqa, dka, dva,
    retk, retq, ink, inq, dqs, dkvs,
    loc_sem, keep_sem, ready,
    qd_s, qd_r, kv_s, kv_r, st_s, st_r,
    zq_s, zq_r, zk_s, zk_r, zst_s, zst_r,
    rk_s, rk_r, rq_s, rq_r, oq_s, oq_r, okv_s, okv_r,
):
    U, B = uly_count, blk_count
    T = q_hbm.shape[0]
    R = T * U
    D = HEAD_SIZE
    GD = GROUP * D
    H = R // 2
    bf, f32 = jnp.bfloat16, jnp.float32
    scale = 1.0 / math.sqrt(D)
    u = lax.axis_index("uly")
    b = lax.axis_index("blk")
    has_dn = b >= 1
    has_up = b + 1 < B
    mid = jnp.logical_and(has_dn, has_up)

    def at(blk, uly):
        return {"blk": blk, "uly": uly}

    def rcopy(src, dst, ssem, rsem, dev):
        return pltpu.make_async_remote_copy(
            src_ref=src, dst_ref=dst, send_sem=ssem, recv_sem=rsem,
            device_id=dev, device_id_type=pl.DeviceIdType.MESH,
        )

    def cols(first, width):
        return pl.ds(pl.multiple_of(first, 128), width)

    def rows(place, base=0):
        return pl.ds(pl.multiple_of(base + place * T, T), T)

    def each(low, high, step):
        def body(i, c):
            step(i)
            return c
        lax.fori_loop(low, high, body, 0)

    barrier = pltpu.get_barrier_semaphore()
    for k in range(1, U):
        pl.semaphore_signal(
            barrier, inc=1, device_id=at(b, lax.rem(u + k, U)), device_id_type=pl.DeviceIdType.MESH
        )

    @pl.when(has_dn)
    def _():
        pl.semaphore_signal(barrier, inc=1, device_id=at(b - 1, u), device_id_type=pl.DeviceIdType.MESH)

    loads = [
        pltpu.make_async_copy(src, dst, loc_sem.at[i])
        for i, (src, dst) in enumerate([
            (q_hbm, q_in), (do_hbm, do_in), (k_hbm, k_in), (v_hbm, v_in),
            (out_hbm, out_in), (lp_hbm, lp_in), (ids_hbm, ids_in),
        ])
    ]
    own = [
        pltpu.make_async_copy(q_hbm.at[:, cols(u * GD, GD)], qb.at[rows(u), :], loc_sem.at[7]),
        pltpu.make_async_copy(do_hbm.at[:, cols(u * GD, GD)], dob.at[rows(u), :], loc_sem.at[8]),
        pltpu.make_async_copy(k_hbm.at[:, cols(u * D, D)], kvb.at[0, rows(u), :], loc_sem.at[9]),
        pltpu.make_async_copy(v_hbm.at[:, cols(u * D, D)], kvb.at[1, rows(u), :], loc_sem.at[10]),
    ]
    for copy in loads + own:
        copy.start()

    def clear(i):
        spot = pl.ds(pl.multiple_of(i * T, T), T)
        dqa[0, spot, :] = jnp.zeros((T, D), f32)
        dqa[1, spot, :] = jnp.zeros((T, D), f32)
        dka[:, spot] = jnp.zeros((D, T), f32)
        dva[:, spot] = jnp.zeros((D, T), f32)
        kaug[:, spot] = jnp.zeros((D, T), bf)

    each(0, 2 * U, clear)
    r8 = lax.broadcasted_iota(jnp.int32, (8, T), 0)
    ones_v = jnp.where(jnp.logical_and(r8 >= 4, r8 < 7), 1.0, 0.0)
    for i in range(H // T):
        vaug[:, i * T:(i + 1) * T] = jnp.concatenate(
            [ones_v, jnp.zeros((D - 8, T), f32)], axis=0
        ).astype(bf)

    for copy in loads[:4]:
        copy.wait()
    pl.semaphore_wait(barrier, U - 1 + has_up.astype(jnp.int32))

    @pl.when(has_up)
    def _():
        pl.semaphore_signal(ready, inc=1, device_id=at(b + 1, u), device_id_type=pl.DeviceIdType.MESH)

    def frm_of(k):
        return lax.rem(u + U - k, U)

    def qd_in(which, h, k, place, peer, dev):
        ref, buf = ((q_in, qb), (do_in, dob))[which]
        return rcopy(
            ref.at[:, cols(peer * GD + h * D, D)], buf.at[rows(place), h * D:(h + 1) * D],
            qd_s.at[0], qd_r.at[h, k], dev,
        )

    def kv_in(which, k, place, peer, dev):
        ref = (k_in, v_in)[which]
        return rcopy(
            ref.at[:, cols(peer * D, D)], kvb.at[which, rows(place), :],
            kv_s.at[0], kv_r.at[k], dev,
        )

    def st_in(k, place, peer, dev):
        return rcopy(stat_ref.at[peer], statb.at[0, place], st_s.at[0], st_r.at[0], dev)

    def many(height, width, sem):
        part = qb.at[pl.ds(0, height * width // GD), :]
        pltpu.make_async_copy(part, part, sem).wait()

    def stat_wait(sem):
        part = statb.at[0, pl.ds(0, U - 1)]
        pltpu.make_async_copy(part, part, sem).wait()

    def send_qd(h):
        def one(k):
            to = lax.rem(u + k, U)
            for which in range(2):
                qd_in(which, h, k, u, to, at(b, to)).start()
        each(1, U, one)

    def send_kv(k):
        to = lax.rem(u + k, U)
        for which in range(2):
            kv_in(which, k, u, to, at(b, to)).start()

    send_qd(0)
    each(1, U, send_kv)

    for copy in loads[4:]:
        copy.wait()
    lane = lax.broadcasted_iota(jnp.int32, (T, 128), 1)
    table = jnp.zeros((T, 128), f32)
    for h in range(QUERY_HEADS):
        piece = slice(h * D, (h + 1) * D)
        total = jnp.sum(
            do_in[:, piece].astype(f32) * out_in[:, piece].astype(f32), axis=1, keepdims=True
        )
        table = jnp.where(lane == h, total, table)
    table = table.T
    part0, part1 = lp_in[:, 0, :], lp_in[:, 1, :]
    highest = jnp.maximum(part0, part1)
    lse_rows = highest + jnp.log(jnp.exp(part0 - highest) + jnp.exp(part1 - highest))
    id_rows = jnp.broadcast_to(ids_in[...].astype(f32), (8 - 2 * GROUP, T))
    for p in range(U):
        pick = slice(p * GROUP, (p + 1) * GROUP)
        stat_ref[p] = jnp.concatenate([lse_rows[pick], table[pick], id_rows], axis=0)
    statb[0, u] = stat_ref[u]

    def send_st(k):
        to = lax.rem(u + k, U)
        st_in(k, u, to, at(b, to)).start()

    each(1, U, send_st)
    send_qd(1)

    def zq(which, h, place):
        buf = (qb, dob)[which]
        return rcopy(
            buf.at[rows(place), h * D:(h + 1) * D], buf.at[rows(place, R), h * D:(h + 1) * D],
            zq_s.at[0], zq_r.at[h], at(b - 1, u),
        )

    def zk(which, place):
        return rcopy(
            kvb.at[which, rows(place), :], kvb.at[which, rows(place, R), :],
            zk_s.at[0], zk_r.at[0], at(b + 1, u),
        )

    def zst(which):
        dev = (at(b - 1, u), at(b + 1, u))[which]
        return rcopy(statb.at[0], statb.at[1 + which], zst_s.at[which], zst_r.at[which], dev)

    lower = b >= 2
    late = lax.rem(b, LAYER) == 0
    late_q = jnp.logical_and(lower, late)

    def relay_q(h, place):
        @pl.when(jnp.logical_and(lower, jnp.logical_not(late)) if h == 0 else lower)
        def _():
            for which in range(2):
                zq(which, h, place).start()

    def relay_k(place):
        @pl.when(has_up)
        def _():
            for which in range(2):
                zk(which, place).start()

    def turn_q(h, base):
        def one(p):
            spot = rows(p, base)
            qT[h, :, spot] = qb[spot, h * D:(h + 1) * D].T
            dT[h, :, spot] = dob[spot, h * D:(h + 1) * D].T
        each(0, U, one)

    def turn_k(base):
        def one(p):
            spot = rows(p, base)
            kT[:, spot] = kvb[0, spot, :].T
            vT[:, spot] = kvb[1, spot, :].T
        each(0, U, one)

    def codes(st):
        doc = jnp.broadcast_to(st[4:5, :], (16, T))
        high = jnp.floor(doc * 0.125)
        low = (doc - 8.0 * high)[:8]
        i16 = lax.broadcasted_iota(jnp.int32, (16, T), 0).astype(f32)
        return jnp.where(i16[:8] == low, 1.0, 0.0), jnp.where(i16 == high, 1.0, 0.0)

    def split3(x):
        a = x.astype(bf).astype(f32)
        c = (x - a).astype(bf).astype(f32)
        return a, c, (x - a - c)

    def build_q(which):
        def one(p):
            st = statb[which, p]
            oc, oa = codes(st)
            for h in range(GROUP):
                rows8 = jnp.ones((8, T), f32)
                parts = split3(st[h:h + 1, :] * (-math.sqrt(D)))
                more = split3(-st[GROUP + h:GROUP + h + 1, :])
                for i in range(3):
                    rows8 = jnp.where(r8 == i, parts[i], rows8)
                    rows8 = jnp.where(r8 == 4 + i, more[i], rows8)
                full = jnp.concatenate([rows8, oc, oa, jnp.zeros((D - 32, T), f32)], axis=0)
                aug[h, rows(p, which * R), :] = full.T.astype(bf)
        each(0, U, one)

    def build_k(src, base):
        def one(p):
            oc, oa = codes(statb[src, p])
            rows8 = jnp.where(r8 < 3, 1.0, jnp.where(r8 == 3, -2.0 * FAR, 0.0))
            kaug[0:32, rows(p, base)] = jnp.concatenate(
                [rows8, oc * FAR, oa * FAR], axis=0
            ).astype(bf)
        each(0, U, one)

    own[0].wait()
    own[1].wait()

    @pl.when(jnp.logical_and(has_dn, jnp.logical_not(late)))
    def _():
        pl.semaphore_wait(ready, 1)

    relay_q(0, u)

    def got_q(h):
        def one(k):
            frm = frm_of(k)
            many(2 * T, D, qd_r.at[h, k])
            relay_q(h, frm)
        each(1, U, one)

    got_q(0)
    own[2].wait()
    own[3].wait()
    relay_k(u)
    turn_q(0, 0)

    @pl.when(jnp.logical_and(has_dn, late))
    def _():
        pl.semaphore_wait(ready, 1)

    @pl.when(late_q)
    def _():
        def one(p):
            for which in range(2):
                zq(which, 0, p).start()
        each(0, U, one)

    relay_q(1, u)

    def got_k(k):
        many(2 * T, D, kv_r.at[k])
        relay_k(frm_of(k))

    each(1, U, got_k)
    turn_k(0)
    stat_wait(st_r.at[0])

    @pl.when(lower)
    def _():
        zst(0).start()

    @pl.when(has_up)
    def _():
        zst(1).start()

    build_q(0)
    build_k(0, 0)

    factor = scale * math.log2(math.e)

    def tile(qi, ki, causal, heads=(0, 1)):
        qrow = pl.ds(pl.multiple_of(qi * H, H), H)
        krow = pl.ds(pl.multiple_of(ki * H, H), H)
        ks = jnp.concatenate([kT[:, krow], kaug[:, krow]], axis=0)
        vs = jnp.concatenate([vT[:, krow], vaug[...]], axis=0)
        kn = kvb[0, krow, :]
        dk = dv = None
        for h in heads:
            extra = aug[h, qrow, :]
            qs = jnp.concatenate([qb[qrow, h * D:(h + 1) * D], extra], axis=1)
            ds = jnp.concatenate([dob[qrow, h * D:(h + 1) * D], extra], axis=1)
            w = jnp.exp2(dot(qs, ks) * factor)
            if causal:
                qpos = lax.broadcasted_iota(jnp.int32, (H, H), 0) + qi * H
                kpos = lax.broadcasted_iota(jnp.int32, (H, H), 1) + ki * H
                w = jnp.where(kpos <= qpos, w, 0.0)
            g = (w * dot(ds, vs)).astype(bf)
            w = w.astype(bf)
            part_v = dot(dT[h, :, qrow], w)
            part_k = dot(qT[h, :, qrow], g)
            dqa[h, qrow, :] += dot(g, kn)
            dv = part_v if dv is None else dv + part_v
            dk = part_k if dk is None else dk + part_k
        dva[:, krow] += dv
        dka[:, krow] += dk

    each(0, 3, lambda t: tile((t + 1) // 2, t // 2, True, (0,)))
    got_q(1)
    turn_q(1, 0)
    each(0, 3, lambda t: tile((t + 1) // 2, t // 2, True, (1,)))

    def give_k(half, which):
        return rcopy(
            retk.at[half, which], ink.at[half, which],
            rk_s.at[half, which], rk_r.at[half, which], at(b - 1, u),
        )

    def give_q(half, h):
        return rcopy(
            retq.at[half, h], inq.at[half, h],
            rq_s.at[half, h], rq_r.at[half, h], at(b + 1, u),
        )

    def half_of(half, base=0):
        return slice(base + half * H, base + (half + 1) * H)

    def return_k(which, half):
        total = (dka, dva)[which]
        retk[half, which] = total[:, half_of(half, R)].astype(bf)
        give_k(half, which).start()

    def return_q(half, h):
        retq[half, h] = dqa[h, half_of(half, R), :].astype(bf)
        give_q(half, h).start()

    @pl.when(has_dn)
    def _():
        zst(1).wait_recv()
        many(2 * R, D, zk_r.at[0])
        turn_k(R)
        build_k(2, R)
        each(0, 4, lambda t: tile(t % 2, 3 - t // 2, False))

    @pl.when(mid)
    def _():
        zst(0).wait_recv()
        build_q(1)
        for h in range(GROUP):
            many(2 * R, D, zq_r.at[h])
            turn_q(h, R)

        def far(t):
            tile(3 - (t + 1) // 2, 3 - t // 2, False)

            @pl.when(t == 0)
            def _():
                for h in range(GROUP):
                    return_q(1, h)

            @pl.when(t == 1)
            def _():
                return_k(1, 1)

        each(0, 3, far)
        return_q(0, 0)
        return_k(1, 0)
        return_q(0, 1)
        return_k(0, 1)
        return_k(0, 0)

    @pl.when(jnp.logical_and(has_dn, jnp.logical_not(has_up)))
    def _():
        for which in (1, 0):
            for half in (1, 0):
                return_k(which, half)

    def oq(h, place, peer, dev):
        return rcopy(
            dqs.at[rows(place), h * D:(h + 1) * D], dq_ref.at[:, cols(peer * GD + h * D, D)],
            oq_s.at[0], oq_r.at[0], dev,
        )

    def okv(which, place, peer, dev):
        ref = (dk_ref, dv_ref)[which]
        return rcopy(
            dkvs.at[which, rows(place), :], ref.at[:, cols(peer * D, D)],
            okv_s.at[0], okv_r.at[which], dev,
        )

    def keep_q(h):
        return pltpu.make_async_copy(
            dqs.at[rows(u), h * D:(h + 1) * D], dq_ref.at[:, cols(u * GD + h * D, D)],
            keep_sem.at[2 + h],
        )

    def keep_kv(which):
        ref = (dk_ref, dv_ref)[which]
        return pltpu.make_async_copy(
            dkvs.at[which, rows(u), :], ref.at[:, cols(u * D, D)], keep_sem.at[which]
        )

    def finish_q(h):
        @pl.when(lower)
        def _():
            for half in (1, 0):
                give_q(half, h).wait_recv()
                dqa[h, half_of(half), :] += inq[half, h].astype(f32)
        dqs[:, h * D:(h + 1) * D] = (dqa[h, 0:R, :] * scale).astype(bf)

        def go(k):
            to = lax.rem(u + k, U)
            oq(h, to, u, at(b, to)).start()

        each(1, U, go)
        keep_q(h).start()

    def finish_kv(which):
        total = (dka, dva)[which]

        @pl.when(has_up)
        def _():
            for half in (1, 0):
                give_k(half, which).wait_recv()
                total[:, half_of(half)] += ink[half, which].astype(f32)
        for half in (1, 0):
            value = total[:, half_of(half)]
            if which == 0:
                value = value * scale
            dkvs[which, half_of(half), :] = value.T.astype(bf)

        def go(k):
            to = lax.rem(u + k, U)
            okv(which, to, u, at(b, to)).start()

        each(1, U, go)
        keep_kv(which).start()

    finish_q(0)
    finish_kv(1)
    finish_q(1)
    finish_kv(0)
    for h in range(GROUP):
        keep_q(h).wait()
    for which in range(2):
        keep_kv(which).wait()

    many((U - 1) * 4 * T, D, qd_s.at[0])
    many((U - 1) * 2 * T, D, kv_s.at[0])
    stat_wait(st_s.at[0])

    @pl.when(lower)
    def _():
        zst(0).wait_send()
        many(4 * R, D, zq_s.at[0])

    @pl.when(has_up)
    def _():
        zst(1).wait_send()
        many(2 * R, D, zk_s.at[0])

    @pl.when(has_dn)
    def _():
        for half in range(2):
            for which in range(2):
                give_k(half, which).wait_send()

    @pl.when(mid)
    def _():
        for half in range(2):
            for h in range(GROUP):
                give_q(half, h).wait_send()

    many((U - 1) * T, GD, oq_s.at[0])
    many((U - 1) * 2 * T, D, okv_s.at[0])
    many((U - 1) * T, GD, oq_r.at[0])
    for which in range(2):
        many((U - 1) * T, D, okv_r.at[which])


def close_kernel(a_in, b_in, c_in, a_out, b_out, c_out, a_mid, b_mid, c_mid, in_sem, out_sem):
    moves = []
    for i, (src, mid, dst) in enumerate(
        [(a_in, a_mid, a_out), (b_in, b_mid, b_out), (c_in, c_mid, c_out)]
    ):
        height = src.shape[0] // PIECES
        for n in range(PIECES):
            part = pl.ds(n * height, height)
            moves.append((
                pltpu.make_async_copy(src.at[part], mid.at[part], in_sem.at[i, n]),
                pltpu.make_async_copy(mid.at[part], dst.at[part], out_sem.at[i, n]),
            ))
    for load, _ in moves:
        load.start()
    for load, store in moves:
        load.wait()
        store.start()
    for _, store in moves:
        store.wait()


def per_device(uly_count, blk_count, q, k, v, out, grad, lse_parts, segment_ids):
    U, B = uly_count, blk_count
    T = q.shape[0]
    R = T * U
    D = HEAD_SIZE
    GD = GROUP * D
    assert KEY_VALUE_HEADS == U
    parts = lse_parts.transpose(1, 2, 0)
    ids = segment_ids.reshape(1, T)
    bf, f32 = jnp.bfloat16, jnp.float32
    dma = pltpu.SemaphoreType.DMA
    sems = []
    for sent, got in [
        ((1,), (GROUP, U)), ((1,), (U,)), ((1,), (1,)), ((1,), (GROUP,)), ((1,), (1,)),
        ((2,), (2,)), ((2, 2), (2, 2)), ((2, 2), (2, 2)), ((1,), (1,)), ((1,), (2,)),
    ]:
        sems += [dma(sent), dma(got)]
    vm = pltpu.VMEM
    results = pl.pallas_call(
        functools.partial(kernel, U, B),
        out_shape=(
            jax.ShapeDtypeStruct(q.shape, bf),
            jax.ShapeDtypeStruct(k.shape, bf),
            jax.ShapeDtypeStruct(v.shape, bf),
        ),
        in_specs=[pl.BlockSpec(memory_space=pltpu.HBM)] * 7,
        out_specs=tuple([pl.BlockSpec(memory_space=pltpu.HBM)] * 3),
        scratch_shapes=[
            vm(q.shape, bf), vm(q.shape, bf), vm(k.shape, bf), vm(v.shape, bf),
            vm(q.shape, bf), vm(parts.shape, f32), vm((1, T), jnp.int32),
            vm((2 * R, GD), bf), vm((2 * R, GD), bf), vm((2, 2 * R, D), bf),
            vm((U, 8, T), f32), vm((3, U, 8, T), f32),
            vm((GROUP, 2 * R, D), bf), vm((D, 2 * R), bf), vm((D, R // 2), bf),
            vm((GROUP, D, 2 * R), bf), vm((GROUP, D, 2 * R), bf),
            vm((D, 2 * R), bf), vm((D, 2 * R), bf),
            vm((GROUP, 2 * R, D), f32), vm((D, 2 * R), f32), vm((D, 2 * R), f32),
            vm((2, 2, D, R // 2), bf), vm((2, GROUP, R // 2, D), bf),
            vm((2, 2, D, R // 2), bf), vm((2, GROUP, R // 2, D), bf),
            vm((R, GD), bf), vm((2, R, D), bf),
            dma((11,)), dma((4,)), pltpu.SemaphoreType.REGULAR,
        ] + sems,
        compiler_params=pltpu.CompilerParams(
            collective_id=0, has_side_effects=True, vmem_limit_bytes=60 << 20
        ),
    )(q, grad, k, v, out, parts, ids)
    hbm = [pl.BlockSpec(memory_space=pltpu.HBM)] * 3
    return pl.pallas_call(
        close_kernel,
        out_shape=tuple(jax.ShapeDtypeStruct(r.shape, r.dtype) for r in results),
        in_specs=hbm,
        out_specs=tuple(hbm),
        scratch_shapes=[vm(r.shape, r.dtype) for r in results]
        + [dma((3, PIECES)), dma((3, PIECES))],
        compiler_params=pltpu.CompilerParams(vmem_limit_bytes=56 << 20),
    )(*results)


def solution(mesh):
    spec = P(("blk", "uly"), None)
    body = functools.partial(per_device, mesh.shape["uly"], mesh.shape["blk"])
    return jax.shard_map(
        body,
        mesh=mesh,
        in_specs=(spec, spec, spec, spec, spec, P(("blk", "uly"), None, None), P(("blk", "uly"))),
        out_specs=(spec, spec, spec),
        check_vma=False,
    )
```

```python
import functools
import math

import jax
import jax.numpy as jnp
from jax import lax
from jax.experimental import pallas as pl
from jax.experimental.pallas import tpu as pltpu
from jax.sharding import PartitionSpec as P

HEAD_SIZE = 128
QUERY_HEADS = 16
KEY_VALUE_HEADS = 8
GROUP = QUERY_HEADS // KEY_VALUE_HEADS
PIECES = 2
FAR = 8192.0
LAYER = 16
UNROLL = 4


def dot(a, b):
    return lax.dot_general(a, b, (((1,), (0,)), ((), ())), preferred_element_type=jnp.float32)


def kernel(
    uly_count, blk_count,
    q_hbm, do_hbm, k_hbm, v_hbm, out_hbm, lp_hbm, ids_hbm,
    dq_ref, dk_ref, dv_ref,
    q_in, do_in, k_in, v_in, out_in, lp_in, ids_in,
    qb, dob, kvb, stat_ref, statb,
    aug, kaug, vaug, qT, dT, kT, vT,
    dqa, dka, dva,
    retk, retq, ink, inq, dqs, dkvs,
    loc_sem, keep_sem, ready,
    qd_s, qd_r, kv_s, kv_r, st_s, st_r,
    zq_s, zq_r, zk_s, zk_r, zst_s, zst_r,
    rk_s, rk_r, rq_s, rq_r, oq_s, oq_r, okv_s, okv_r,
):
    U, B = uly_count, blk_count
    T = q_hbm.shape[0]
    R = T * U
    D = HEAD_SIZE
    GD = GROUP * D
    H = R // 2
    bf, f32 = jnp.bfloat16, jnp.float32
    scale = 1.0 / math.sqrt(D)
    u = lax.axis_index("uly")
    b = lax.axis_index("blk")
    has_dn = b >= 1
    has_up = b + 1 < B
    mid = jnp.logical_and(has_dn, has_up)

    def at(blk, uly):
        return {"blk": blk, "uly": uly}

    def rcopy(src, dst, ssem, rsem, dev):
        return pltpu.make_async_remote_copy(
            src_ref=src, dst_ref=dst, send_sem=ssem, recv_sem=rsem,
            device_id=dev, device_id_type=pl.DeviceIdType.MESH,
        )

    def cols(first, width):
        return pl.ds(pl.multiple_of(first, 128), width)

    def rows(place, base=0):
        return pl.ds(pl.multiple_of(base + place * T, T), T)

    def each(low, high, step, unroll=1):
        def body(i, c):
            step(i)
            return c
        lax.fori_loop(low, high, body, 0, unroll=unroll)

    barrier = pltpu.get_barrier_semaphore()
    for k in range(1, U):
        pl.semaphore_signal(
            barrier, inc=1, device_id=at(b, lax.rem(u + k, U)), device_id_type=pl.DeviceIdType.MESH
        )

    @pl.when(has_dn)
    def _():
        pl.semaphore_signal(barrier, inc=1, device_id=at(b - 1, u), device_id_type=pl.DeviceIdType.MESH)

    loads = [
        pltpu.make_async_copy(src, dst, loc_sem.at[i])
        for i, (src, dst) in enumerate([
            (q_hbm, q_in), (do_hbm, do_in), (k_hbm, k_in), (v_hbm, v_in),
            (out_hbm, out_in), (lp_hbm, lp_in), (ids_hbm, ids_in),
        ])
    ]
    own = [
        pltpu.make_async_copy(q_hbm.at[:, cols(u * GD, GD)], qb.at[rows(u), :], loc_sem.at[7]),
        pltpu.make_async_copy(do_hbm.at[:, cols(u * GD, GD)], dob.at[rows(u), :], loc_sem.at[8]),
        pltpu.make_async_copy(k_hbm.at[:, cols(u * D, D)], kvb.at[0, rows(u), :], loc_sem.at[9]),
        pltpu.make_async_copy(v_hbm.at[:, cols(u * D, D)], kvb.at[1, rows(u), :], loc_sem.at[10]),
    ]
    for copy in loads + own:
        copy.start()

    def clear(i):
        spot = pl.ds(pl.multiple_of(i * T, T), T)
        dqa[0, spot, :] = jnp.zeros((T, D), f32)
        dqa[1, spot, :] = jnp.zeros((T, D), f32)
        dka[:, spot] = jnp.zeros((D, T), f32)
        dva[:, spot] = jnp.zeros((D, T), f32)
        kaug[:, spot] = jnp.zeros((D, T), bf)

    each(0, 2 * U, clear)
    r8 = lax.broadcasted_iota(jnp.int32, (8, T), 0)
    ones_v = jnp.where(jnp.logical_and(r8 >= 4, r8 < 7), 1.0, 0.0)
    for i in range(H // T):
        vaug[:, i * T:(i + 1) * T] = jnp.concatenate(
            [ones_v, jnp.zeros((D - 8, T), f32)], axis=0
        ).astype(bf)

    for copy in loads[:4]:
        copy.wait()
    pl.semaphore_wait(barrier, U - 1 + has_up.astype(jnp.int32))

    @pl.when(has_up)
    def _():
        pl.semaphore_signal(ready, inc=1, device_id=at(b + 1, u), device_id_type=pl.DeviceIdType.MESH)

    def frm_of(k):
        return lax.rem(u + U - k, U)

    def qd_in(which, h, k, place, peer, dev):
        ref, buf = ((q_in, qb), (do_in, dob))[which]
        return rcopy(
            ref.at[:, cols(peer * GD + h * D, D)], buf.at[rows(place), h * D:(h + 1) * D],
            qd_s.at[0], qd_r.at[h, k], dev,
        )

    def kv_in(which, k, place, peer, dev):
        ref = (k_in, v_in)[which]
        return rcopy(
            ref.at[:, cols(peer * D, D)], kvb.at[which, rows(place), :],
            kv_s.at[0], kv_r.at[k], dev,
        )

    def st_in(k, place, peer, dev):
        return rcopy(stat_ref.at[peer], statb.at[0, place], st_s.at[0], st_r.at[0], dev)

    def many(height, width, sem):
        part = qb.at[pl.ds(0, height * width // GD), :]
        pltpu.make_async_copy(part, part, sem).wait()

    def stat_wait(sem):
        part = statb.at[0, pl.ds(0, U - 1)]
        pltpu.make_async_copy(part, part, sem).wait()

    def send_qd(h):
        def one(k):
            to = lax.rem(u + k, U)
            for which in range(2):
                qd_in(which, h, k, u, to, at(b, to)).start()
        each(1, U, one)

    def send_kv(k):
        to = lax.rem(u + k, U)
        for which in range(2):
            kv_in(which, k, u, to, at(b, to)).start()

    send_qd(0)

    for copy in loads[4:]:
        copy.wait()
    lane = lax.broadcasted_iota(jnp.int32, (T, 128), 1)
    table = jnp.zeros((T, 128), f32)
    for h in range(QUERY_HEADS):
        piece = slice(h * D, (h + 1) * D)
        total = jnp.sum(
            do_in[:, piece].astype(f32) * out_in[:, piece].astype(f32), axis=1, keepdims=True
        )
        table = jnp.where(lane == h, total, table)
    table = table.T
    part0, part1 = lp_in[:, 0, :], lp_in[:, 1, :]
    highest = jnp.maximum(part0, part1)
    lse_rows = highest + jnp.log(jnp.exp(part0 - highest) + jnp.exp(part1 - highest))
    id_rows = jnp.broadcast_to(ids_in[...].astype(f32), (8 - 2 * GROUP, T))
    for p in range(U):
        pick = slice(p * GROUP, (p + 1) * GROUP)
        stat_ref[p] = jnp.concatenate([lse_rows[pick], table[pick], id_rows], axis=0)
    statb[0, u] = stat_ref[u]

    def send_st(k):
        to = lax.rem(u + k, U)
        st_in(k, u, to, at(b, to)).start()

    each(1, U, send_st)
    each(1, U, send_kv)
    send_qd(1)

    def zq(which, h, place):
        buf = (qb, dob)[which]
        return rcopy(
            buf.at[rows(place), h * D:(h + 1) * D], buf.at[rows(place, R), h * D:(h + 1) * D],
            zq_s.at[0], zq_r.at[h], at(b - 1, u),
        )

    def zk(which, place):
        return rcopy(
            kvb.at[which, rows(place), :], kvb.at[which, rows(place, R), :],
            zk_s.at[0], zk_r.at[0], at(b + 1, u),
        )

    def zst(which):
        dev = (at(b - 1, u), at(b + 1, u))[which]
        return rcopy(statb.at[0], statb.at[1 + which], zst_s.at[which], zst_r.at[which], dev)

    lower = b >= 2
    late = lax.rem(b, LAYER) == 0
    late_q = jnp.logical_and(lower, late)

    def relay_q(h, place):
        @pl.when(jnp.logical_and(lower, jnp.logical_not(late)) if h == 0 else lower)
        def _():
            for which in range(2):
                zq(which, h, place).start()

    def relay_k(place):
        @pl.when(has_up)
        def _():
            for which in range(2):
                zk(which, place).start()

    def turn_q(h, base):
        def one(p):
            spot = rows(p, base)
            qT[h, :, spot] = qb[spot, h * D:(h + 1) * D].T
            dT[h, :, spot] = dob[spot, h * D:(h + 1) * D].T
        each(0, U, one, UNROLL)

    def turn_k(base):
        def one(p):
            spot = rows(p, base)
            kT[:, spot] = kvb[0, spot, :].T
            vT[:, spot] = kvb[1, spot, :].T
        each(0, U, one, UNROLL)

    def codes(st):
        doc = jnp.broadcast_to(st[4:5, :], (16, T))
        high = jnp.floor(doc * 0.125)
        low = (doc - 8.0 * high)[:8]
        i16 = lax.broadcasted_iota(jnp.int32, (16, T), 0).astype(f32)
        return jnp.where(i16[:8] == low, 1.0, 0.0), jnp.where(i16 == high, 1.0, 0.0)

    def split3(x):
        a = x.astype(bf).astype(f32)
        c = (x - a).astype(bf).astype(f32)
        return a, c, (x - a - c)

    def build_q(which):
        def one(p):
            st = statb[which, p]
            oc, oa = codes(st)
            for h in range(GROUP):
                rows8 = jnp.ones((8, T), f32)
                parts = split3(st[h:h + 1, :] * (-math.sqrt(D)))
                more = split3(-st[GROUP + h:GROUP + h + 1, :])
                for i in range(3):
                    rows8 = jnp.where(r8 == i, parts[i], rows8)
                    rows8 = jnp.where(r8 == 4 + i, more[i], rows8)
                full = jnp.concatenate([rows8, oc, oa, jnp.zeros((D - 32, T), f32)], axis=0)
                aug[h, rows(p, which * R), :] = full.T.astype(bf)
        each(0, U, one, UNROLL)

    def build_k(src, base):
        def one(p):
            oc, oa = codes(statb[src, p])
            rows8 = jnp.where(r8 < 3, 1.0, jnp.where(r8 == 3, -2.0 * FAR, 0.0))
            kaug[0:32, rows(p, base)] = jnp.concatenate(
                [rows8, oc * FAR, oa * FAR], axis=0
            ).astype(bf)
        each(0, U, one, UNROLL)

    own[0].wait()
    own[1].wait()

    @pl.when(jnp.logical_and(has_dn, jnp.logical_not(late)))
    def _():
        pl.semaphore_wait(ready, 1)

    relay_q(0, u)

    def got_q(h):
        def one(k):
            frm = frm_of(k)
            many(2 * T, D, qd_r.at[h, k])
            relay_q(h, frm)
        each(1, U, one)

    got_q(0)
    own[2].wait()
    own[3].wait()
    relay_k(u)
    turn_q(0, 0)

    @pl.when(jnp.logical_and(has_dn, late))
    def _():
        pl.semaphore_wait(ready, 1)

    @pl.when(late_q)
    def _():
        def one(p):
            for which in range(2):
                zq(which, 0, p).start()
        each(0, U, one)

    relay_q(1, u)

    def got_k(k):
        many(2 * T, D, kv_r.at[k])
        relay_k(frm_of(k))

    each(1, U, got_k)
    turn_k(0)
    stat_wait(st_r.at[0])

    @pl.when(lower)
    def _():
        zst(0).start()

    @pl.when(has_up)
    def _():
        zst(1).start()

    build_q(0)
    build_k(0, 0)

    factor = scale * math.log2(math.e)

    def tile(qi, ki, causal, heads=(0, 1)):
        qrow = pl.ds(pl.multiple_of(qi * H, H), H)
        krow = pl.ds(pl.multiple_of(ki * H, H), H)
        ks = jnp.concatenate([kT[:, krow], kaug[:, krow]], axis=0)
        vs = jnp.concatenate([vT[:, krow], vaug[...]], axis=0)
        kn = kvb[0, krow, :]
        dk = dv = None
        raw = []
        for h in heads:
            extra = aug[h, qrow, :]
            qs = jnp.concatenate([qb[qrow, h * D:(h + 1) * D], extra], axis=1)
            ds = jnp.concatenate([dob[qrow, h * D:(h + 1) * D], extra], axis=1)
            raw.append((dot(qs, ks), dot(ds, vs)))
        for h, (score, prob) in zip(heads, raw):
            w = jnp.exp2(score * factor)
            if causal:
                qpos = lax.broadcasted_iota(jnp.int32, (H, H), 0) + qi * H
                kpos = lax.broadcasted_iota(jnp.int32, (H, H), 1) + ki * H
                w = jnp.where(kpos <= qpos, w, 0.0)
            g = (w * prob).astype(bf)
            w = w.astype(bf)
            part_v = dot(dT[h, :, qrow], w)
            part_k = dot(qT[h, :, qrow], g)
            dqa[h, qrow, :] += dot(g, kn)
            dv = part_v if dv is None else dv + part_v
            dk = part_k if dk is None else dk + part_k
        dva[:, krow] += dv
        dka[:, krow] += dk

    each(0, 3, lambda t: tile((t + 1) // 2, t // 2, True, (0,)))
    got_q(1)
    turn_q(1, 0)
    each(0, 3, lambda t: tile((t + 1) // 2, t // 2, True, (1,)))

    def give_k(half, which):
        return rcopy(
            retk.at[half, which], ink.at[half, which],
            rk_s.at[half, which], rk_r.at[half, which], at(b - 1, u),
        )

    def give_q(half, h):
        return rcopy(
            retq.at[half, h], inq.at[half, h],
            rq_s.at[half, h], rq_r.at[half, h], at(b + 1, u),
        )

    def half_of(half, base=0):
        return slice(base + half * H, base + (half + 1) * H)

    def return_k(which, half):
        total = (dka, dva)[which]
        retk[half, which] = total[:, half_of(half, R)].astype(bf)
        give_k(half, which).start()

    def return_q(half, h):
        retq[half, h] = dqa[h, half_of(half, R), :].astype(bf)
        give_q(half, h).start()

    def take_next():
        zst(0).wait_recv()
        build_q(1)
        for h in range(GROUP):
            many(2 * R, D, zq_r.at[h])
            turn_q(h, R)

    def pick(t, table):
        out = table[0]
        for i, value in enumerate(table[1:]):
            out = jnp.where(t > i, value, out)
        return out

    late_i, mid_i = late.astype(jnp.int32), mid.astype(jnp.int32)
    edge = lax.rem(b, LAYER) == LAYER - 1
    first_c = jnp.where(edge, 2, 3) * (1 - late_i)
    last_c = first_c + 2
    last = 3 + 3 * mid_i
    last_v = jnp.where(edge, 1 + 2 * mid_i, 4)

    @pl.when(has_dn)
    def _():
        zst(1).wait_recv()
        many(2 * R, D, zk_r.at[0])
        turn_k(R)
        build_k(2, R)

        def step(t):
            @pl.when(jnp.logical_and(mid, t == first_c))
            def _():
                take_next()

            c = t - first_c
            is_c = jnp.logical_and(mid, jnp.logical_and(c >= 0, c < 3))
            n = t - jnp.where(jnp.logical_and(mid, c >= 3), 3, 0)
            qi = jnp.where(is_c, pick(c, (3, 2, 2)), n % 2)
            ki = jnp.where(is_c, pick(c, (3, 3, 2)), 3 - n // 2)
            tile(qi, ki, False)

            @pl.when(jnp.logical_and(mid, t == first_c))
            def _():
                return_q(1, 0)

            @pl.when(jnp.logical_and(mid, t == last_c))
            def _():
                return_q(0, 0)
                return_q(1, 1)
                return_q(0, 1)

            @pl.when(t == last_v)
            def _():
                return_k(1, 1)

            @pl.when(t == last)
            def _():
                return_k(1, 0)
                return_k(0, 1)
                return_k(0, 0)

        each(0, last + 1, step)

    def oq(h, place, peer, dev):
        return rcopy(
            dqs.at[rows(place), h * D:(h + 1) * D], dq_ref.at[:, cols(peer * GD + h * D, D)],
            oq_s.at[0], oq_r.at[0], dev,
        )

    def okv(which, place, peer, dev):
        ref = (dk_ref, dv_ref)[which]
        return rcopy(
            dkvs.at[which, rows(place), :], ref.at[:, cols(peer * D, D)],
            okv_s.at[0], okv_r.at[which], dev,
        )

    def keep_q(h):
        return pltpu.make_async_copy(
            dqs.at[rows(u), h * D:(h + 1) * D], dq_ref.at[:, cols(u * GD + h * D, D)],
            keep_sem.at[2 + h],
        )

    def keep_kv(which):
        ref = (dk_ref, dv_ref)[which]
        return pltpu.make_async_copy(
            dkvs.at[which, rows(u), :], ref.at[:, cols(u * D, D)], keep_sem.at[which]
        )

    def finish_q(h):
        @pl.when(lower)
        def _():
            for half in (1, 0):
                give_q(half, h).wait_recv()
                dqa[h, half_of(half), :] += inq[half, h].astype(f32)
        dqs[:, h * D:(h + 1) * D] = (dqa[h, 0:R, :] * scale).astype(bf)

        def go(k):
            to = lax.rem(u + k, U)
            oq(h, to, u, at(b, to)).start()

        each(1, U, go)
        keep_q(h).start()

    def finish_kv(which):
        total = (dka, dva)[which]

        @pl.when(has_up)
        def _():
            for half in (1, 0):
                give_k(half, which).wait_recv()
                total[:, half_of(half)] += ink[half, which].astype(f32)
        for half in (1, 0):
            value = total[:, half_of(half)]
            if which == 0:
                value = value * scale
            dkvs[which, half_of(half), :] = value.T.astype(bf)

        def go(k):
            to = lax.rem(u + k, U)
            okv(which, to, u, at(b, to)).start()

        each(1, U, go)
        keep_kv(which).start()

    @pl.when(jnp.logical_not(late))
    def _():
        finish_q(0)

    finish_kv(1)

    @pl.when(jnp.logical_not(late))
    def _():
        finish_q(1)

    finish_kv(0)

    @pl.when(late)
    def _():
        for h in range(GROUP):
            finish_q(h)

    many((U - 1) * 4 * T, D, qd_s.at[0])
    many((U - 1) * 2 * T, D, kv_s.at[0])
    stat_wait(st_s.at[0])

    @pl.when(lower)
    def _():
        zst(0).wait_send()
        many(4 * R, D, zq_s.at[0])

    @pl.when(has_up)
    def _():
        zst(1).wait_send()
        many(2 * R, D, zk_s.at[0])

    @pl.when(has_dn)
    def _():
        for half in range(2):
            for which in range(2):
                give_k(half, which).wait_send()

    @pl.when(mid)
    def _():
        for half in range(2):
            for h in range(GROUP):
                give_q(half, h).wait_send()

    for h in range(GROUP):
        keep_q(h).wait()
    for which in range(2):
        keep_kv(which).wait()
    many((U - 1) * T, GD, oq_s.at[0])
    many((U - 1) * 2 * T, D, okv_s.at[0])
    many((U - 1) * T, GD, oq_r.at[0])
    for which in range(2):
        many((U - 1) * T, D, okv_r.at[which])


def close_kernel(a_in, b_in, c_in, a_out, b_out, c_out, a_mid, b_mid, c_mid, in_sem, out_sem):
    moves = []
    for i, (src, mid, dst) in enumerate(
        [(a_in, a_mid, a_out), (b_in, b_mid, b_out), (c_in, c_mid, c_out)]
    ):
        height = src.shape[0] // PIECES
        for n in range(PIECES):
            part = pl.ds(n * height, height)
            moves.append((
                pltpu.make_async_copy(src.at[part], mid.at[part], in_sem.at[i, n]),
                pltpu.make_async_copy(mid.at[part], dst.at[part], out_sem.at[i, n]),
            ))
    for load, _ in moves:
        load.start()
    for load, store in moves:
        load.wait()
        store.start()
    for _, store in moves:
        store.wait()


def per_device(uly_count, blk_count, q, k, v, out, grad, lse_parts, segment_ids):
    U, B = uly_count, blk_count
    T = q.shape[0]
    R = T * U
    D = HEAD_SIZE
    GD = GROUP * D
    assert KEY_VALUE_HEADS == U
    parts = lse_parts.transpose(1, 2, 0)
    ids = segment_ids.reshape(1, T)
    bf, f32 = jnp.bfloat16, jnp.float32
    dma = pltpu.SemaphoreType.DMA
    sems = []
    for sent, got in [
        ((1,), (GROUP, U)), ((1,), (U,)), ((1,), (1,)), ((1,), (GROUP,)), ((1,), (1,)),
        ((2,), (2,)), ((2, 2), (2, 2)), ((2, 2), (2, 2)), ((1,), (1,)), ((1,), (2,)),
    ]:
        sems += [dma(sent), dma(got)]
    vm = pltpu.VMEM
    results = pl.pallas_call(
        functools.partial(kernel, U, B),
        out_shape=(
            jax.ShapeDtypeStruct(q.shape, bf),
            jax.ShapeDtypeStruct(k.shape, bf),
            jax.ShapeDtypeStruct(v.shape, bf),
        ),
        in_specs=[pl.BlockSpec(memory_space=pltpu.HBM)] * 7,
        out_specs=tuple([pl.BlockSpec(memory_space=pltpu.HBM)] * 3),
        scratch_shapes=[
            vm(q.shape, bf), vm(q.shape, bf), vm(k.shape, bf), vm(v.shape, bf),
            vm(q.shape, bf), vm(parts.shape, f32), vm((1, T), jnp.int32),
            vm((2 * R, GD), bf), vm((2 * R, GD), bf), vm((2, 2 * R, D), bf),
            vm((U, 8, T), f32), vm((3, U, 8, T), f32),
            vm((GROUP, 2 * R, D), bf), vm((D, 2 * R), bf), vm((D, R // 2), bf),
            vm((GROUP, D, 2 * R), bf), vm((GROUP, D, 2 * R), bf),
            vm((D, 2 * R), bf), vm((D, 2 * R), bf),
            vm((GROUP, 2 * R, D), f32), vm((D, 2 * R), f32), vm((D, 2 * R), f32),
            vm((2, 2, D, R // 2), bf), vm((2, GROUP, R // 2, D), bf),
            vm((2, 2, D, R // 2), bf), vm((2, GROUP, R // 2, D), bf),
            vm((R, GD), bf), vm((2, R, D), bf),
            dma((11,)), dma((4,)), pltpu.SemaphoreType.REGULAR,
        ] + sems,
        compiler_params=pltpu.CompilerParams(
            collective_id=0, has_side_effects=True, vmem_limit_bytes=60 << 20
        ),
    )(q, grad, k, v, out, parts, ids)
    hbm = [pl.BlockSpec(memory_space=pltpu.HBM)] * 3
    return pl.pallas_call(
        close_kernel,
        out_shape=tuple(jax.ShapeDtypeStruct(r.shape, r.dtype) for r in results),
        in_specs=hbm,
        out_specs=tuple(hbm),
        scratch_shapes=[vm(r.shape, r.dtype) for r in results]
        + [dma((3, PIECES)), dma((3, PIECES))],
        compiler_params=pltpu.CompilerParams(vmem_limit_bytes=56 << 20),
    )(*results)


def solution(mesh):
    spec = P(("blk", "uly"), None)
    body = functools.partial(per_device, mesh.shape["uly"], mesh.shape["blk"])
    return jax.shard_map(
        body,
        mesh=mesh,
        in_specs=(spec, spec, spec, spec, spec, P(("blk", "uly"), None, None), P(("blk", "uly"))),
        out_specs=(spec, spec, spec),
        check_vma=False,
    )
```

```python
import functools
import math

import jax
import jax.numpy as jnp
from jax import lax
from jax.experimental import pallas as pl
from jax.experimental.pallas import tpu as pltpu
from jax.sharding import PartitionSpec as P

HEAD_SIZE = 128
QUERY_HEADS = 16
KEY_VALUE_HEADS = 8
GROUP = QUERY_HEADS // KEY_VALUE_HEADS
PIECES = 2
FAR = 8192.0
LAYER = 16
UNROLL = 4


def dot(a, b):
    return lax.dot_general(a, b, (((1,), (0,)), ((), ())), preferred_element_type=jnp.float32)


def kernel(
    uly_count, blk_count,
    q_hbm, do_hbm, k_hbm, v_hbm, out_hbm, lp_hbm, ids_hbm,
    dq_ref, dk_ref, dv_ref,
    q_in, do_in, k_in, v_in, out_in, lp_in, ids_in,
    qb, dob, kvb, stat_ref, statb,
    aug, kaug, vaug, qT, dT, kT, vT,
    dqa, dka, dva,
    retk, retq, ink, inq, dqs, dkvs,
    loc_sem, ready,
    qd_s, qd_r, kv_s, kv_r, st_s, st_r,
    zq_s, zq_r, zk_s, zk_r, zst_s, zst_r,
    rk_s, rk_r, rq_s, rq_r, oq_s, oq_r, okv_s, okv_r,
):
    U, B = uly_count, blk_count
    T = q_hbm.shape[0]
    R = T * U
    D = HEAD_SIZE
    GD = GROUP * D
    H = R // 2
    bf, f32 = jnp.bfloat16, jnp.float32
    scale = 1.0 / math.sqrt(D)
    u = lax.axis_index("uly")
    b = lax.axis_index("blk")
    has_dn = b >= 1
    has_up = b + 1 < B
    mid = jnp.logical_and(has_dn, has_up)

    def at(blk, uly):
        return {"blk": blk, "uly": uly}

    def rcopy(src, dst, ssem, rsem, dev):
        return pltpu.make_async_remote_copy(
            src_ref=src, dst_ref=dst, send_sem=ssem, recv_sem=rsem,
            device_id=dev, device_id_type=pl.DeviceIdType.MESH,
        )

    def cols(first, width):
        return pl.ds(pl.multiple_of(first, 128), width)

    def rows(place, base=0):
        return pl.ds(pl.multiple_of(base + place * T, T), T)

    def each(low, high, step, unroll=1):
        def body(i, c):
            step(i)
            return c
        lax.fori_loop(low, high, body, 0, unroll=unroll)

    barrier = pltpu.get_barrier_semaphore()
    for k in range(1, U):
        pl.semaphore_signal(
            barrier, inc=1, device_id=at(b, lax.rem(u + k, U)), device_id_type=pl.DeviceIdType.MESH
        )

    @pl.when(has_dn)
    def _():
        pl.semaphore_signal(barrier, inc=1, device_id=at(b - 1, u), device_id_type=pl.DeviceIdType.MESH)

    loads = [
        pltpu.make_async_copy(src, dst, loc_sem.at[i])
        for i, (src, dst) in enumerate([
            (q_hbm, q_in), (do_hbm, do_in), (k_hbm, k_in), (v_hbm, v_in),
            (out_hbm, out_in), (lp_hbm, lp_in), (ids_hbm, ids_in),
        ])
    ]
    own = [
        pltpu.make_async_copy(q_hbm.at[:, cols(u * GD, GD)], qb.at[rows(u), :], loc_sem.at[7]),
        pltpu.make_async_copy(do_hbm.at[:, cols(u * GD, GD)], dob.at[rows(u), :], loc_sem.at[8]),
        pltpu.make_async_copy(k_hbm.at[:, cols(u * D, D)], kvb.at[0, rows(u), :], loc_sem.at[9]),
        pltpu.make_async_copy(v_hbm.at[:, cols(u * D, D)], kvb.at[1, rows(u), :], loc_sem.at[10]),
    ]
    for copy in loads + own:
        copy.start()

    def clear(i):
        spot = pl.ds(pl.multiple_of(i * T, T), T)
        dqa[0, spot, :] = jnp.zeros((T, D), f32)
        dqa[1, spot, :] = jnp.zeros((T, D), f32)
        dka[:, spot] = jnp.zeros((D, T), f32)
        dva[:, spot] = jnp.zeros((D, T), f32)
        kaug[:, spot] = jnp.zeros((D, T), bf)

    each(0, 2 * U, clear)
    r8 = lax.broadcasted_iota(jnp.int32, (8, T), 0)
    ones_v = jnp.where(jnp.logical_and(r8 >= 4, r8 < 7), 1.0, 0.0)
    for i in range(H // T):
        vaug[:, i * T:(i + 1) * T] = jnp.concatenate(
            [ones_v, jnp.zeros((D - 8, T), f32)], axis=0
        ).astype(bf)

    for copy in loads[:4]:
        copy.wait()
    pl.semaphore_wait(barrier, U - 1 + has_up.astype(jnp.int32))

    @pl.when(has_up)
    def _():
        pl.semaphore_signal(ready, inc=1, device_id=at(b + 1, u), device_id_type=pl.DeviceIdType.MESH)

    def frm_of(k):
        return lax.rem(u + U - k, U)

    def qd_in(which, h, k, place, peer, dev):
        ref, buf = ((q_in, qb), (do_in, dob))[which]
        return rcopy(
            ref.at[:, cols(peer * GD + h * D, D)], buf.at[rows(place), h * D:(h + 1) * D],
            qd_s.at[0], qd_r.at[h, k], dev,
        )

    def kv_in(which, k, place, peer, dev):
        ref = (k_in, v_in)[which]
        return rcopy(
            ref.at[:, cols(peer * D, D)], kvb.at[which, rows(place), :],
            kv_s.at[0], kv_r.at[k], dev,
        )

    def st_in(k, place, peer, dev):
        return rcopy(stat_ref.at[peer], statb.at[0, place], st_s.at[0], st_r.at[0], dev)

    def many(height, width, sem):
        part = qb.at[pl.ds(0, height * width // GD), :]
        pltpu.make_async_copy(part, part, sem).wait()

    def stat_wait(sem):
        part = statb.at[0, pl.ds(0, U - 1)]
        pltpu.make_async_copy(part, part, sem).wait()

    def send_qd(h):
        def one(k):
            to = lax.rem(u + k, U)
            for which in range(2):
                qd_in(which, h, k, u, to, at(b, to)).start()
        each(1, U, one)

    def send_kv(k):
        to = lax.rem(u + k, U)
        for which in range(2):
            kv_in(which, k, u, to, at(b, to)).start()

    send_qd(0)

    for copy in loads[4:]:
        copy.wait()
    lane = lax.broadcasted_iota(jnp.int32, (T, 128), 1)
    table = jnp.zeros((T, 128), f32)
    for h in range(QUERY_HEADS):
        piece = slice(h * D, (h + 1) * D)
        total = jnp.sum(
            do_in[:, piece].astype(f32) * out_in[:, piece].astype(f32), axis=1, keepdims=True
        )
        table = jnp.where(lane == h, total, table)
    table = table.T
    part0, part1 = lp_in[:, 0, :], lp_in[:, 1, :]
    highest = jnp.maximum(part0, part1)
    lse_rows = highest + jnp.log(jnp.exp(part0 - highest) + jnp.exp(part1 - highest))
    id_rows = jnp.broadcast_to(ids_in[...].astype(f32), (8 - 2 * GROUP, T))
    for p in range(U):
        pick = slice(p * GROUP, (p + 1) * GROUP)
        stat_ref[p] = jnp.concatenate([lse_rows[pick], table[pick], id_rows], axis=0)
    statb[0, u] = stat_ref[u]

    def send_st(k):
        to = lax.rem(u + k, U)
        st_in(k, u, to, at(b, to)).start()

    each(1, U, send_st)
    each(1, U, send_kv)
    send_qd(1)

    def zq(which, h, place):
        buf = (qb, dob)[which]
        return rcopy(
            buf.at[rows(place), h * D:(h + 1) * D], buf.at[rows(place, R), h * D:(h + 1) * D],
            zq_s.at[0], zq_r.at[h], at(b - 1, u),
        )

    def zk(which, place):
        return rcopy(
            kvb.at[which, rows(place), :], kvb.at[which, rows(place, R), :],
            zk_s.at[0], zk_r.at[0], at(b + 1, u),
        )

    def zst(which):
        dev = (at(b - 1, u), at(b + 1, u))[which]
        return rcopy(statb.at[0], statb.at[1 + which], zst_s.at[which], zst_r.at[which], dev)

    lower = b >= 2
    late = lax.rem(b, LAYER) == 0
    late_q = jnp.logical_and(lower, late)

    def relay_q(h, place):
        @pl.when(jnp.logical_and(lower, jnp.logical_not(late)) if h == 0 else lower)
        def _():
            for which in range(2):
                zq(which, h, place).start()

    def relay_k(place):
        @pl.when(has_up)
        def _():
            for which in range(2):
                zk(which, place).start()

    def turn_q(h, base):
        def one(p):
            spot = rows(p, base)
            qT[h, :, spot] = qb[spot, h * D:(h + 1) * D].T
            dT[h, :, spot] = dob[spot, h * D:(h + 1) * D].T
        each(0, U, one, UNROLL)

    def turn_k(base):
        def one(p):
            spot = rows(p, base)
            kT[:, spot] = kvb[0, spot, :].T
            vT[:, spot] = kvb[1, spot, :].T
        each(0, U, one, UNROLL)

    def codes(st):
        doc = jnp.broadcast_to(st[4:5, :], (16, T))
        high = jnp.floor(doc * 0.125)
        low = (doc - 8.0 * high)[:8]
        i16 = lax.broadcasted_iota(jnp.int32, (16, T), 0).astype(f32)
        return jnp.where(i16[:8] == low, 1.0, 0.0), jnp.where(i16 == high, 1.0, 0.0)

    def split3(x):
        a = x.astype(bf).astype(f32)
        c = (x - a).astype(bf).astype(f32)
        return a, c, (x - a - c)

    def build_q(which):
        def one(p):
            st = statb[which, p]
            oc, oa = codes(st)
            for h in range(GROUP):
                rows8 = jnp.ones((8, T), f32)
                parts = split3(st[h:h + 1, :] * (-math.sqrt(D)))
                more = split3(-st[GROUP + h:GROUP + h + 1, :])
                for i in range(3):
                    rows8 = jnp.where(r8 == i, parts[i], rows8)
                    rows8 = jnp.where(r8 == 4 + i, more[i], rows8)
                full = jnp.concatenate([rows8, oc, oa, jnp.zeros((D - 32, T), f32)], axis=0)
                aug[h, rows(p, which * R), :] = full.T.astype(bf)
        each(0, U, one, UNROLL)

    def build_k(src, base):
        def one(p):
            oc, oa = codes(statb[src, p])
            rows8 = jnp.where(r8 < 3, 1.0, jnp.where(r8 == 3, -2.0 * FAR, 0.0))
            kaug[0:32, rows(p, base)] = jnp.concatenate(
                [rows8, oc * FAR, oa * FAR], axis=0
            ).astype(bf)
        each(0, U, one, UNROLL)

    own[0].wait()
    own[1].wait()

    @pl.when(jnp.logical_and(has_dn, jnp.logical_not(late)))
    def _():
        pl.semaphore_wait(ready, 1)

    relay_q(0, u)

    def got_q(h):
        def one(k):
            frm = frm_of(k)
            many(2 * T, D, qd_r.at[h, k])
            relay_q(h, frm)
        each(1, U, one)

    got_q(0)
    own[2].wait()
    own[3].wait()
    relay_k(u)
    turn_q(0, 0)

    @pl.when(jnp.logical_and(has_dn, late))
    def _():
        pl.semaphore_wait(ready, 1)

    @pl.when(late_q)
    def _():
        def one(p):
            for which in range(2):
                zq(which, 0, p).start()
        each(0, U, one)

    relay_q(1, u)

    def got_k(k):
        many(2 * T, D, kv_r.at[k])
        relay_k(frm_of(k))

    each(1, U, got_k)
    turn_k(0)
    stat_wait(st_r.at[0])

    @pl.when(lower)
    def _():
        zst(0).start()

    @pl.when(has_up)
    def _():
        zst(1).start()

    build_q(0)
    build_k(0, 0)

    factor = scale * math.log2(math.e)

    def tile(qi, ki, causal, heads=(0, 1)):
        qrow = pl.ds(pl.multiple_of(qi * H, H), H)
        krow = pl.ds(pl.multiple_of(ki * H, H), H)
        ks = jnp.concatenate([kT[:, krow], kaug[:, krow]], axis=0)
        vs = jnp.concatenate([vT[:, krow], vaug[...]], axis=0)
        kn = kvb[0, krow, :]
        dk = dv = None
        raw = []
        for h in heads:
            extra = aug[h, qrow, :]
            qs = jnp.concatenate([qb[qrow, h * D:(h + 1) * D], extra], axis=1)
            ds = jnp.concatenate([dob[qrow, h * D:(h + 1) * D], extra], axis=1)
            raw.append((dot(qs, ks), dot(ds, vs)))
        for h, (score, prob) in zip(heads, raw):
            w = jnp.exp2(score * factor)
            if causal:
                qpos = lax.broadcasted_iota(jnp.int32, (H, H), 0) + qi * H
                kpos = lax.broadcasted_iota(jnp.int32, (H, H), 1) + ki * H
                w = jnp.where(kpos <= qpos, w, 0.0)
            g = (w * prob).astype(bf)
            w = w.astype(bf)
            part_v = dot(dT[h, :, qrow], w)
            part_k = dot(qT[h, :, qrow], g)
            dqa[h, qrow, :] += dot(g, kn)
            dv = part_v if dv is None else dv + part_v
            dk = part_k if dk is None else dk + part_k
        dva[:, krow] += dv
        dka[:, krow] += dk

    each(0, 3, lambda t: tile((t + 1) // 2, t // 2, True, (0,)))
    got_q(1)
    turn_q(1, 0)
    each(0, 3, lambda t: tile((t + 1) // 2, t // 2, True, (1,)))

    def give_k(half, which):
        return rcopy(
            retk.at[half, which], ink.at[half, which],
            rk_s.at[half, which], rk_r.at[half, which], at(b - 1, u),
        )

    def give_q(half, h):
        return rcopy(
            retq.at[half, h], inq.at[half, h],
            rq_s.at[half, h], rq_r.at[half, h], at(b + 1, u),
        )

    def half_of(half, base=0):
        return slice(base + half * H, base + (half + 1) * H)

    def return_k(which, half):
        total = (dka, dva)[which]
        retk[half, which] = total[:, half_of(half, R)].astype(bf)
        give_k(half, which).start()

    def return_q(half, h):
        retq[half, h] = dqa[h, half_of(half, R), :].astype(bf)
        give_q(half, h).start()

    def take_next():
        zst(0).wait_recv()
        build_q(1)
        for h in range(GROUP):
            many(2 * R, D, zq_r.at[h])
            turn_q(h, R)

    def pick(t, table):
        out = table[0]
        for i, value in enumerate(table[1:]):
            out = jnp.where(t > i, value, out)
        return out

    late_i, mid_i = late.astype(jnp.int32), mid.astype(jnp.int32)
    edge = lax.rem(b, LAYER) == LAYER - 1
    first_c = jnp.where(edge, 2, 3) * (1 - late_i)
    last_c = first_c + 2
    last = 3 + 3 * mid_i
    last_v = jnp.where(edge, 1 + 2 * mid_i, 4)

    @pl.when(has_dn)
    def _():
        zst(1).wait_recv()
        many(2 * R, D, zk_r.at[0])
        turn_k(R)
        build_k(2, R)

        def step(t):
            @pl.when(jnp.logical_and(mid, t == first_c))
            def _():
                take_next()

            c = t - first_c
            is_c = jnp.logical_and(mid, jnp.logical_and(c >= 0, c < 3))
            n = t - jnp.where(jnp.logical_and(mid, c >= 3), 3, 0)
            qi = jnp.where(is_c, pick(c, (3, 2, 2)), n % 2)
            ki = jnp.where(is_c, pick(c, (3, 3, 2)), 3 - n // 2)
            tile(qi, ki, False)

            @pl.when(jnp.logical_and(mid, t == first_c))
            def _():
                return_q(1, 0)

            @pl.when(jnp.logical_and(mid, t == last_c))
            def _():
                return_q(0, 0)
                return_q(1, 1)
                return_q(0, 1)

            @pl.when(t == last_v)
            def _():
                return_k(1, 1)

            @pl.when(t == last)
            def _():
                return_k(1, 0)
                return_k(0, 1)
                return_k(0, 0)

        each(0, last + 1, step)

    def oq(h, place, peer, dev):
        return rcopy(
            dqs.at[rows(place), h * D:(h + 1) * D], dq_ref.at[:, cols(peer * GD + h * D, D)],
            oq_s.at[0], oq_r.at[0], dev,
        )

    def okv(which, place, peer, dev):
        ref = (dk_ref, dv_ref)[which]
        return rcopy(
            dkvs.at[which, rows(place), :], ref.at[:, cols(peer * D, D)],
            okv_s.at[0], okv_r.at[which], dev,
        )

    def finish_q(h):
        @pl.when(lower)
        def _():
            for half in (1, 0):
                give_q(half, h).wait_recv()
                dqa[h, half_of(half), :] += inq[half, h].astype(f32)
        dqs[:, h * D:(h + 1) * D] = (dqa[h, 0:R, :] * scale).astype(bf)

        def go(k):
            to = lax.rem(u + k, U)
            oq(h, to, u, at(b, to)).start()

        each(1, U, go)
        dq_ref[:, cols(u * GD + h * D, D)] = dqs[rows(u), h * D:(h + 1) * D]

    def finish_kv(which):
        total = (dka, dva)[which]

        @pl.when(has_up)
        def _():
            for half in (1, 0):
                give_k(half, which).wait_recv()
                total[:, half_of(half)] += ink[half, which].astype(f32)
        for half in (1, 0):
            value = total[:, half_of(half)]
            if which == 0:
                value = value * scale
            dkvs[which, half_of(half), :] = value.T.astype(bf)

        def go(k):
            to = lax.rem(u + k, U)
            okv(which, to, u, at(b, to)).start()

        each(1, U, go)
        (dk_ref, dv_ref)[which][:, cols(u * D, D)] = dkvs[which, rows(u), :]

    @pl.when(jnp.logical_not(late))
    def _():
        finish_q(0)

    finish_kv(1)

    @pl.when(jnp.logical_not(late))
    def _():
        finish_q(1)

    finish_kv(0)

    @pl.when(late)
    def _():
        for h in range(GROUP):
            finish_q(h)

    many((U - 1) * 4 * T, D, qd_s.at[0])
    many((U - 1) * 2 * T, D, kv_s.at[0])
    stat_wait(st_s.at[0])

    @pl.when(lower)
    def _():
        zst(0).wait_send()
        many(4 * R, D, zq_s.at[0])

    @pl.when(has_up)
    def _():
        zst(1).wait_send()
        many(2 * R, D, zk_s.at[0])

    @pl.when(has_dn)
    def _():
        for half in range(2):
            for which in range(2):
                give_k(half, which).wait_send()

    @pl.when(mid)
    def _():
        for half in range(2):
            for h in range(GROUP):
                give_q(half, h).wait_send()

    many((U - 1) * T, GD, oq_s.at[0])
    many((U - 1) * 2 * T, D, okv_s.at[0])
    many((U - 1) * T, GD, oq_r.at[0])
    for which in range(2):
        many((U - 1) * T, D, okv_r.at[which])


def close_kernel(a_in, b_in, c_in, a_out, b_out, c_out, sem):
    moves = [
        pltpu.make_async_copy(src, dst, sem.at[i])
        for i, (src, dst) in enumerate([(a_in, a_out), (b_in, b_out), (c_in, c_out)])
    ]
    for move in moves:
        move.start()
    for move in moves:
        move.wait()


def per_device(uly_count, blk_count, q, k, v, out, grad, lse_parts, segment_ids):
    U, B = uly_count, blk_count
    T = q.shape[0]
    R = T * U
    D = HEAD_SIZE
    GD = GROUP * D
    assert KEY_VALUE_HEADS == U
    parts = lse_parts.transpose(1, 2, 0)
    ids = segment_ids.reshape(1, T)
    bf, f32 = jnp.bfloat16, jnp.float32
    dma = pltpu.SemaphoreType.DMA
    sems = []
    for sent, got in [
        ((1,), (GROUP, U)), ((1,), (U,)), ((1,), (1,)), ((1,), (GROUP,)), ((1,), (1,)),
        ((2,), (2,)), ((2, 2), (2, 2)), ((2, 2), (2, 2)), ((1,), (1,)), ((1,), (2,)),
    ]:
        sems += [dma(sent), dma(got)]
    vm = pltpu.VMEM
    results = pl.pallas_call(
        functools.partial(kernel, U, B),
        out_shape=(
            pltpu.VMEM(q.shape, bf),
            pltpu.VMEM(k.shape, bf),
            pltpu.VMEM(v.shape, bf),
        ),
        in_specs=[pl.BlockSpec(memory_space=pltpu.HBM)] * 7,
        out_specs=tuple([pl.BlockSpec(memory_space=pltpu.VMEM)] * 3),
        scratch_shapes=[
            vm(q.shape, bf), vm(q.shape, bf), vm(k.shape, bf), vm(v.shape, bf),
            vm(q.shape, bf), vm(parts.shape, f32), vm((1, T), jnp.int32),
            vm((2 * R, GD), bf), vm((2 * R, GD), bf), vm((2, 2 * R, D), bf),
            vm((U, 8, T), f32), vm((3, U, 8, T), f32),
            vm((GROUP, 2 * R, D), bf), vm((D, 2 * R), bf), vm((D, R // 2), bf),
            vm((GROUP, D, 2 * R), bf), vm((GROUP, D, 2 * R), bf),
            vm((D, 2 * R), bf), vm((D, 2 * R), bf),
            vm((GROUP, 2 * R, D), f32), vm((D, 2 * R), f32), vm((D, 2 * R), f32),
            vm((2, 2, D, R // 2), bf), vm((2, GROUP, R // 2, D), bf),
            vm((2, 2, D, R // 2), bf), vm((2, GROUP, R // 2, D), bf),
            vm((R, GD), bf), vm((2, R, D), bf),
            dma((11,)), pltpu.SemaphoreType.REGULAR,
        ] + sems,
        compiler_params=pltpu.CompilerParams(
            collective_id=0, has_side_effects=True, vmem_limit_bytes=60 << 20
        ),
    )(q, grad, k, v, out, parts, ids)
    hbm = [pl.BlockSpec(memory_space=pltpu.HBM)] * 3
    return pl.pallas_call(
        close_kernel,
        out_shape=tuple(jax.ShapeDtypeStruct(r.shape, r.dtype) for r in results),
        in_specs=[pl.BlockSpec(memory_space=pltpu.VMEM)] * 3,
        out_specs=tuple(hbm),
        scratch_shapes=[dma((3,))],
        compiler_params=pltpu.CompilerParams(vmem_limit_bytes=8 << 20),
    )(*results)


def solution(mesh):
    spec = P(("blk", "uly"), None)
    body = functools.partial(per_device, mesh.shape["uly"], mesh.shape["blk"])
    return jax.shard_map(
        body,
        mesh=mesh,
        in_specs=(spec, spec, spec, spec, spec, P(("blk", "uly"), None, None), P(("blk", "uly"))),
        out_specs=(spec, spec, spec),
        check_vma=False,
    )
```

```python
import functools
import math

import jax
import jax.numpy as jnp
from jax import lax
from jax.experimental import pallas as pl
from jax.experimental.pallas import tpu as pltpu
from jax.sharding import PartitionSpec as P

HEAD_SIZE = 128
QUERY_HEADS = 16
KEY_VALUE_HEADS = 8
GROUP = QUERY_HEADS // KEY_VALUE_HEADS
PIECES = 2
FAR = 8192.0
LAYER = 16
UNROLL = 4


def dot(a, b):
    return lax.dot_general(a, b, (((1,), (0,)), ((), ())), preferred_element_type=jnp.float32)


def kernel(
    uly_count, blk_count,
    q_hbm, do_hbm, k_hbm, v_hbm, out_hbm, lp_hbm, ids_hbm,
    dq_ref, dk_ref, dv_ref,
    q_in, do_in, k_in, v_in, out_in, lp_in, ids_in,
    qb, dob, kvb, stat_ref, statb,
    aug, kaug, vaug, qT, dT, kT, vT,
    dqa, dka, dva,
    retk, retq, ink, inq, dqs, dkvs,
    loc_sem, ready,
    qd_s, qd_r, kv_s, kv_r, st_s, st_r,
    zq_s, zq_r, zk_s, zk_r, zst_s, zst_r,
    rk_s, rk_r, rq_s, rq_r, oq_s, oq_r, okv_s, okv_r,
):
    U, B = uly_count, blk_count
    T = q_hbm.shape[0]
    R = T * U
    D = HEAD_SIZE
    GD = GROUP * D
    H = R // 2
    bf, f32 = jnp.bfloat16, jnp.float32
    scale = 1.0 / math.sqrt(D)
    u = lax.axis_index("uly")
    b = lax.axis_index("blk")
    has_dn = b >= 1
    has_up = b + 1 < B
    mid = jnp.logical_and(has_dn, has_up)

    def at(blk, uly):
        return {"blk": blk, "uly": uly}

    def rcopy(src, dst, ssem, rsem, dev):
        return pltpu.make_async_remote_copy(
            src_ref=src, dst_ref=dst, send_sem=ssem, recv_sem=rsem,
            device_id=dev, device_id_type=pl.DeviceIdType.MESH,
        )

    def cols(first, width):
        return pl.ds(pl.multiple_of(first, 128), width)

    def rows(place, base=0):
        return pl.ds(pl.multiple_of(base + place * T, T), T)

    def each(low, high, step, unroll=1):
        def body(i, c):
            step(i)
            return c
        lax.fori_loop(low, high, body, 0, unroll=unroll)

    barrier = pltpu.get_barrier_semaphore()
    for k in range(1, U):
        pl.semaphore_signal(
            barrier, inc=1, device_id=at(b, lax.rem(u + k, U)), device_id_type=pl.DeviceIdType.MESH
        )

    @pl.when(has_dn)
    def _():
        pl.semaphore_signal(barrier, inc=1, device_id=at(b - 1, u), device_id_type=pl.DeviceIdType.MESH)

    loads = [
        pltpu.make_async_copy(src, dst, loc_sem.at[i])
        for i, (src, dst) in enumerate([
            (q_hbm, q_in), (do_hbm, do_in), (k_hbm, k_in), (v_hbm, v_in),
            (out_hbm, out_in), (lp_hbm, lp_in), (ids_hbm, ids_in),
        ])
    ]
    own = [
        pltpu.make_async_copy(q_hbm.at[:, cols(u * GD, GD)], qb.at[rows(u), :], loc_sem.at[7]),
        pltpu.make_async_copy(do_hbm.at[:, cols(u * GD, GD)], dob.at[rows(u), :], loc_sem.at[8]),
        pltpu.make_async_copy(k_hbm.at[:, cols(u * D, D)], kvb.at[0, rows(u), :], loc_sem.at[9]),
        pltpu.make_async_copy(v_hbm.at[:, cols(u * D, D)], kvb.at[1, rows(u), :], loc_sem.at[10]),
    ]
    for copy in loads + own:
        copy.start()

    def clear(i):
        spot = pl.ds(pl.multiple_of(i * T, T), T)
        dqa[0, spot, :] = jnp.zeros((T, D), f32)
        dqa[1, spot, :] = jnp.zeros((T, D), f32)
        dka[:, spot] = jnp.zeros((D, T), f32)
        dva[:, spot] = jnp.zeros((D, T), f32)
        kaug[:, spot] = jnp.zeros((D, T), bf)

    each(0, 2 * U, clear)
    r8 = lax.broadcasted_iota(jnp.int32, (8, T), 0)
    ones_v = jnp.where(jnp.logical_and(r8 >= 4, r8 < 7), 1.0, 0.0)
    for i in range(H // T):
        vaug[:, i * T:(i + 1) * T] = jnp.concatenate(
            [ones_v, jnp.zeros((D - 8, T), f32)], axis=0
        ).astype(bf)

    for copy in loads[:4]:
        copy.wait()
    pl.semaphore_wait(barrier, U - 1 + has_up.astype(jnp.int32))

    @pl.when(has_up)
    def _():
        pl.semaphore_signal(ready, inc=1, device_id=at(b + 1, u), device_id_type=pl.DeviceIdType.MESH)

    def frm_of(k):
        return lax.rem(u + U - k, U)

    def qd_in(which, h, k, place, peer, dev):
        ref, buf = ((q_in, qb), (do_in, dob))[which]
        return rcopy(
            ref.at[:, cols(peer * GD + h * D, D)], buf.at[rows(place), h * D:(h + 1) * D],
            qd_s.at[0], qd_r.at[h, k], dev,
        )

    def kv_in(which, k, place, peer, dev):
        ref = (k_in, v_in)[which]
        return rcopy(
            ref.at[:, cols(peer * D, D)], kvb.at[which, rows(place), :],
            kv_s.at[0], kv_r.at[k], dev,
        )

    def st_in(k, place, peer, dev):
        return rcopy(stat_ref.at[peer], statb.at[0, place], st_s.at[0], st_r.at[0], dev)

    def many(height, width, sem):
        part = qb.at[pl.ds(0, height * width // GD), :]
        pltpu.make_async_copy(part, part, sem).wait()

    def stat_wait(sem):
        part = statb.at[0, pl.ds(0, U - 1)]
        pltpu.make_async_copy(part, part, sem).wait()

    def send_qd(h):
        def one(k):
            to = lax.rem(u + k, U)
            for which in range(2):
                qd_in(which, h, k, u, to, at(b, to)).start()
        each(1, U, one)

    def send_kv(k):
        to = lax.rem(u + k, U)
        for which in range(2):
            kv_in(which, k, u, to, at(b, to)).start()

    send_qd(0)

    for copy in loads[4:]:
        copy.wait()
    lane = lax.broadcasted_iota(jnp.int32, (T, 128), 1)
    table = jnp.zeros((T, 128), f32)
    for h in range(QUERY_HEADS):
        piece = slice(h * D, (h + 1) * D)
        total = jnp.sum(
            do_in[:, piece].astype(f32) * out_in[:, piece].astype(f32), axis=1, keepdims=True
        )
        table = jnp.where(lane == h, total, table)
    table = table.T
    part0, part1 = lp_in[:, 0, :], lp_in[:, 1, :]
    highest = jnp.maximum(part0, part1)
    lse_rows = highest + jnp.log(jnp.exp(part0 - highest) + jnp.exp(part1 - highest))
    id_rows = jnp.broadcast_to(ids_in[...].astype(f32), (8 - 2 * GROUP, T))
    for p in range(U):
        pick = slice(p * GROUP, (p + 1) * GROUP)
        stat_ref[p] = jnp.concatenate([lse_rows[pick], table[pick], id_rows], axis=0)
    statb[0, u] = stat_ref[u]

    def send_st(k):
        to = lax.rem(u + k, U)
        st_in(k, u, to, at(b, to)).start()

    each(1, U, send_st)
    each(1, U, send_kv)
    send_qd(1)

    def zq(which, h, place):
        buf = (qb, dob)[which]
        return rcopy(
            buf.at[rows(place), h * D:(h + 1) * D], buf.at[rows(place, R), h * D:(h + 1) * D],
            zq_s.at[0], zq_r.at[h], at(b - 1, u),
        )

    def zk(which, place):
        return rcopy(
            kvb.at[which, rows(place), :], kvb.at[which, rows(place, R), :],
            zk_s.at[0], zk_r.at[0], at(b + 1, u),
        )

    def zst(which):
        dev = (at(b - 1, u), at(b + 1, u))[which]
        return rcopy(statb.at[0], statb.at[1 + which], zst_s.at[which], zst_r.at[which], dev)

    lower = b >= 2
    late = lax.rem(b, LAYER) == 0
    late_q = jnp.logical_and(lower, late)

    def relay_q(h, place):
        @pl.when(jnp.logical_and(lower, jnp.logical_not(late)) if h == 0 else lower)
        def _():
            for which in range(2):
                zq(which, h, place).start()

    def relay_k(place):
        @pl.when(has_up)
        def _():
            for which in range(2):
                zk(which, place).start()

    def turn_q(h, base):
        def one(p):
            spot = rows(p, base)
            qT[h, :, spot] = qb[spot, h * D:(h + 1) * D].T
            dT[h, :, spot] = dob[spot, h * D:(h + 1) * D].T
        each(0, U, one, UNROLL)

    def turn_k(base):
        def one(p):
            spot = rows(p, base)
            kT[:, spot] = kvb[0, spot, :].T
            vT[:, spot] = kvb[1, spot, :].T
        each(0, U, one, UNROLL)

    def codes(st):
        doc = jnp.broadcast_to(st[4:5, :], (16, T))
        high = jnp.floor(doc * 0.125)
        low = (doc - 8.0 * high)[:8]
        i16 = lax.broadcasted_iota(jnp.int32, (16, T), 0).astype(f32)
        return jnp.where(i16[:8] == low, 1.0, 0.0), jnp.where(i16 == high, 1.0, 0.0)

    def split3(x):
        a = x.astype(bf).astype(f32)
        c = (x - a).astype(bf).astype(f32)
        return a, c, (x - a - c)

    def build_q(which):
        def one(p):
            st = statb[which, p]
            oc, oa = codes(st)
            for h in range(GROUP):
                rows8 = jnp.ones((8, T), f32)
                parts = split3(st[h:h + 1, :] * (-math.sqrt(D)))
                more = split3(-st[GROUP + h:GROUP + h + 1, :])
                for i in range(3):
                    rows8 = jnp.where(r8 == i, parts[i], rows8)
                    rows8 = jnp.where(r8 == 4 + i, more[i], rows8)
                full = jnp.concatenate([rows8, oc, oa, jnp.zeros((D - 32, T), f32)], axis=0)
                aug[h, rows(p, which * R), :] = full.T.astype(bf)
        each(0, U, one, UNROLL)

    def build_k(src, base):
        def one(p):
            oc, oa = codes(statb[src, p])
            rows8 = jnp.where(r8 < 3, 1.0, jnp.where(r8 == 3, -2.0 * FAR, 0.0))
            kaug[0:32, rows(p, base)] = jnp.concatenate(
                [rows8, oc * FAR, oa * FAR], axis=0
            ).astype(bf)
        each(0, U, one, UNROLL)

    own[0].wait()
    own[1].wait()

    @pl.when(jnp.logical_and(has_dn, jnp.logical_not(late)))
    def _():
        pl.semaphore_wait(ready, 1)

    relay_q(0, u)

    def got_q(h):
        def one(k):
            frm = frm_of(k)
            many(2 * T, D, qd_r.at[h, k])
            relay_q(h, frm)
        each(1, U, one)

    got_q(0)
    own[2].wait()
    own[3].wait()
    relay_k(u)
    turn_q(0, 0)

    @pl.when(jnp.logical_and(has_dn, late))
    def _():
        pl.semaphore_wait(ready, 1)

    @pl.when(late_q)
    def _():
        def one(p):
            for which in range(2):
                zq(which, 0, p).start()
        each(0, U, one)

    relay_q(1, u)

    def got_k(k):
        many(2 * T, D, kv_r.at[k])
        relay_k(frm_of(k))

    each(1, U, got_k)
    turn_k(0)
    stat_wait(st_r.at[0])

    @pl.when(lower)
    def _():
        zst(0).start()

    @pl.when(has_up)
    def _():
        zst(1).start()

    build_q(0)
    build_k(0, 0)

    factor = scale * math.log2(math.e)

    def tile(qi, ki, causal, heads=(0, 1)):
        qrow = pl.ds(pl.multiple_of(qi * H, H), H)
        krow = pl.ds(pl.multiple_of(ki * H, H), H)
        ks = jnp.concatenate([kT[:, krow], kaug[:, krow]], axis=0)
        vs = jnp.concatenate([vT[:, krow], vaug[...]], axis=0)
        kn = kvb[0, krow, :]
        dk = dv = None
        raw = []
        for h in heads:
            extra = aug[h, qrow, :]
            qs = jnp.concatenate([qb[qrow, h * D:(h + 1) * D], extra], axis=1)
            ds = jnp.concatenate([dob[qrow, h * D:(h + 1) * D], extra], axis=1)
            raw.append((dot(qs, ks), dot(ds, vs)))
        for h, (score, prob) in zip(heads, raw):
            w = jnp.exp2(score * factor)
            if causal:
                qpos = lax.broadcasted_iota(jnp.int32, (H, H), 0) + qi * H
                kpos = lax.broadcasted_iota(jnp.int32, (H, H), 1) + ki * H
                w = jnp.where(kpos <= qpos, w, 0.0)
            g = (w * prob).astype(bf)
            w = w.astype(bf)
            part_v = dot(dT[h, :, qrow], w)
            part_k = dot(qT[h, :, qrow], g)
            dqa[h, qrow, :] += dot(g, kn)
            dv = part_v if dv is None else dv + part_v
            dk = part_k if dk is None else dk + part_k
        dva[:, krow] += dv
        dka[:, krow] += dk

    each(0, 3, lambda t: tile((t + 1) // 2, t // 2, True, (0,)))
    got_q(1)
    turn_q(1, 0)
    each(0, 3, lambda t: tile((t + 1) // 2, t // 2, True, (1,)))

    def give_k(half, which):
        return rcopy(
            retk.at[half, which], ink.at[half, which],
            rk_s.at[half, which], rk_r.at[half, which], at(b - 1, u),
        )

    def give_q(half, h):
        return rcopy(
            retq.at[half, h], inq.at[half, h],
            rq_s.at[half, h], rq_r.at[half, h], at(b + 1, u),
        )

    def half_of(half, base=0):
        return slice(base + half * H, base + (half + 1) * H)

    def return_k(which, half):
        total = (dka, dva)[which]
        retk[half, which] = total[:, half_of(half, R)].astype(bf)
        give_k(half, which).start()

    def return_q(half, h):
        retq[half, h] = dqa[h, half_of(half, R), :].astype(bf)
        give_q(half, h).start()

    def take_next():
        zst(0).wait_recv()
        build_q(1)
        for h in range(GROUP):
            many(2 * R, D, zq_r.at[h])
            turn_q(h, R)

    def pick(t, table):
        out = table[0]
        for i, value in enumerate(table[1:]):
            out = jnp.where(t > i, value, out)
        return out

    late_i, mid_i = late.astype(jnp.int32), mid.astype(jnp.int32)
    edge = lax.rem(b, LAYER) == LAYER - 1
    first_c = jnp.where(edge, 2, 3) * (1 - late_i)
    last_c = first_c + 2
    last = 3 + 3 * mid_i
    last_v = jnp.where(edge, 1 + 2 * mid_i, 4)

    @pl.when(has_dn)
    def _():
        zst(1).wait_recv()
        many(2 * R, D, zk_r.at[0])
        turn_k(R)
        build_k(2, R)

        def step(t):
            @pl.when(jnp.logical_and(mid, t == first_c))
            def _():
                take_next()

            c = t - first_c
            is_c = jnp.logical_and(mid, jnp.logical_and(c >= 0, c < 3))
            n = t - jnp.where(jnp.logical_and(mid, c >= 3), 3, 0)
            qi = jnp.where(is_c, pick(c, (3, 2, 2)), n % 2)
            ki = jnp.where(is_c, pick(c, (3, 3, 2)), 3 - n // 2)
            tile(qi, ki, False)

            @pl.when(jnp.logical_and(mid, t == first_c))
            def _():
                return_q(1, 0)

            @pl.when(jnp.logical_and(mid, t == last_c))
            def _():
                return_q(0, 0)
                return_q(1, 1)
                return_q(0, 1)

            @pl.when(t == last_v)
            def _():
                return_k(1, 1)

            @pl.when(t == last)
            def _():
                return_k(1, 0)
                return_k(0, 1)
                return_k(0, 0)

        each(0, last + 1, step)

    def oq(h, place, peer, dev):
        return rcopy(
            dqs.at[rows(place), h * D:(h + 1) * D], dq_ref.at[:, cols(peer * GD + h * D, D)],
            oq_s.at[0], oq_r.at[0], dev,
        )

    def okv(which, place, peer, dev):
        ref = (dk_ref, dv_ref)[which]
        return rcopy(
            dkvs.at[which, rows(place), :], ref.at[:, cols(peer * D, D)],
            okv_s.at[0], okv_r.at[which], dev,
        )

    def finish_q(h):
        @pl.when(lower)
        def _():
            for half in (1, 0):
                give_q(half, h).wait_recv()
                dqa[h, half_of(half), :] += inq[half, h].astype(f32)
        dqs[:, h * D:(h + 1) * D] = (dqa[h, 0:R, :] * scale).astype(bf)

        def go(k):
            to = lax.rem(u + k, U)
            oq(h, to, u, at(b, to)).start()

        each(1, U, go)
        dq_ref[:, cols(u * GD + h * D, D)] = dqs[rows(u), h * D:(h + 1) * D]

    def finish_kv(which):
        total = (dka, dva)[which]

        @pl.when(has_up)
        def _():
            for half in (1, 0):
                give_k(half, which).wait_recv()
                total[:, half_of(half)] += ink[half, which].astype(f32)
        for half in (1, 0):
            value = total[:, half_of(half)]
            if which == 0:
                value = value * scale
            dkvs[which, half_of(half), :] = value.T.astype(bf)

        def go(k):
            to = lax.rem(u + k, U)
            okv(which, to, u, at(b, to)).start()

        each(1, U, go)
        (dk_ref, dv_ref)[which][:, cols(u * D, D)] = dkvs[which, rows(u), :]

    @pl.when(jnp.logical_not(late))
    def _():
        finish_q(0)

    finish_kv(1)

    @pl.when(late)
    def _():
        finish_q(0)

    @pl.when(jnp.logical_not(late))
    def _():
        finish_q(1)

    finish_kv(0)

    @pl.when(late)
    def _():
        finish_q(1)

    many((U - 1) * 4 * T, D, qd_s.at[0])
    many((U - 1) * 2 * T, D, kv_s.at[0])
    stat_wait(st_s.at[0])

    @pl.when(lower)
    def _():
        zst(0).wait_send()
        many(4 * R, D, zq_s.at[0])

    @pl.when(has_up)
    def _():
        zst(1).wait_send()
        many(2 * R, D, zk_s.at[0])

    @pl.when(has_dn)
    def _():
        for half in range(2):
            for which in range(2):
                give_k(half, which).wait_send()

    @pl.when(mid)
    def _():
        for half in range(2):
            for h in range(GROUP):
                give_q(half, h).wait_send()

    many((U - 1) * T, GD, oq_s.at[0])
    many((U - 1) * 2 * T, D, okv_s.at[0])
    many((U - 1) * T, GD, oq_r.at[0])
    for which in range(2):
        many((U - 1) * T, D, okv_r.at[which])


def close_kernel(a_in, b_in, c_in, a_out, b_out, c_out, sem):
    moves = [
        pltpu.make_async_copy(src, dst, sem.at[i])
        for i, (src, dst) in enumerate([(a_in, a_out), (b_in, b_out), (c_in, c_out)])
    ]
    for move in moves:
        move.start()
    for move in moves:
        move.wait()


def per_device(uly_count, blk_count, q, k, v, out, grad, lse_parts, segment_ids):
    U, B = uly_count, blk_count
    T = q.shape[0]
    R = T * U
    D = HEAD_SIZE
    GD = GROUP * D
    assert KEY_VALUE_HEADS == U
    parts = lse_parts.transpose(1, 2, 0)
    ids = segment_ids.reshape(1, T)
    bf, f32 = jnp.bfloat16, jnp.float32
    dma = pltpu.SemaphoreType.DMA
    sems = []
    for sent, got in [
        ((1,), (GROUP, U)), ((1,), (U,)), ((1,), (1,)), ((1,), (GROUP,)), ((1,), (1,)),
        ((2,), (2,)), ((2, 2), (2, 2)), ((2, 2), (2, 2)), ((1,), (1,)), ((1,), (2,)),
    ]:
        sems += [dma(sent), dma(got)]
    vm = pltpu.VMEM
    results = pl.pallas_call(
        functools.partial(kernel, U, B),
        out_shape=(
            pltpu.VMEM(q.shape, bf),
            pltpu.VMEM(k.shape, bf),
            pltpu.VMEM(v.shape, bf),
        ),
        in_specs=[pl.BlockSpec(memory_space=pltpu.HBM)] * 7,
        out_specs=tuple([pl.BlockSpec(memory_space=pltpu.VMEM)] * 3),
        scratch_shapes=[
            vm(q.shape, bf), vm(q.shape, bf), vm(k.shape, bf), vm(v.shape, bf),
            vm(q.shape, bf), vm(parts.shape, f32), vm((1, T), jnp.int32),
            vm((2 * R, GD), bf), vm((2 * R, GD), bf), vm((2, 2 * R, D), bf),
            vm((U, 8, T), f32), vm((3, U, 8, T), f32),
            vm((GROUP, 2 * R, D), bf), vm((D, 2 * R), bf), vm((D, R // 2), bf),
            vm((GROUP, D, 2 * R), bf), vm((GROUP, D, 2 * R), bf),
            vm((D, 2 * R), bf), vm((D, 2 * R), bf),
            vm((GROUP, 2 * R, D), f32), vm((D, 2 * R), f32), vm((D, 2 * R), f32),
            vm((2, 2, D, R // 2), bf), vm((2, GROUP, R // 2, D), bf),
            vm((2, 2, D, R // 2), bf), vm((2, GROUP, R // 2, D), bf),
            vm((R, GD), bf), vm((2, R, D), bf),
            dma((11,)), pltpu.SemaphoreType.REGULAR,
        ] + sems,
        compiler_params=pltpu.CompilerParams(
            collective_id=0, has_side_effects=True, vmem_limit_bytes=60 << 20
        ),
    )(q, grad, k, v, out, parts, ids)
    hbm = [pl.BlockSpec(memory_space=pltpu.HBM)] * 3
    return pl.pallas_call(
        close_kernel,
        out_shape=tuple(jax.ShapeDtypeStruct(r.shape, r.dtype) for r in results),
        in_specs=[pl.BlockSpec(memory_space=pltpu.VMEM)] * 3,
        out_specs=tuple(hbm),
        scratch_shapes=[dma((3,))],
        compiler_params=pltpu.CompilerParams(vmem_limit_bytes=8 << 20),
    )(*results)


def solution(mesh):
    spec = P(("blk", "uly"), None)
    body = functools.partial(per_device, mesh.shape["uly"], mesh.shape["blk"])
    return jax.shard_map(
        body,
        mesh=mesh,
        in_specs=(spec, spec, spec, spec, spec, P(("blk", "uly"), None, None), P(("blk", "uly"))),
        out_specs=(spec, spec, spec),
        check_vma=False,
    )
```
